128 devices in a mesh: gz: 64 (over y, x, z_hi, core), gy: 2 (over z_lo).
Axes of the slice: x: 4, y: 4, z: 4 (z_hi: 2, z_lo: 2; z = z_hi * 2 + z_lo), core: 2. Of those that a mesh axis runs over, the one named last changes fastest.
Arguments:
- snapshots: float32 [48, 256, 128, 256], P(None, 'gz', 'gy'), may hold values from -6 to 6
- energies: float32 [48], replicated, may hold values from 0.3 to 3
- plane_weight: float32 [256], P('gz'), may hold values from 1 to 10
Outputs:
- modes: float32 [16, 256, 128, 256], P(None, 'gz', 'gy')
- basis: float32 [48, 16], replicated
The draws below stay inside these ranges and needn't reach their ends.
All inputs are finite; a program needn't handle non-finite values.
Results may differ from the reference program's by a relative error of at most 0.0003.
Values sent between devices are 32-bit elements; how exact they have to be, the bound alone decides.
A program may use at most 128 MiB of HBM per device.

```python
import math
import jax
import jax.numpy as jnp
from jax import lax

S = 48
MODES = 16
ITERS = 6
NXF = 256
NY = 128
NZ = 256


def block_levels(own_key, dims, pieces, low, high):
    gain = 1.0
    for position, shards_of in pieces:
        steps = jax.random.uniform(jax.random.fold_in(jax.random.fold_in(own_key, 6), position), (shards_of,), jnp.float32, low / len(pieces), high / len(pieces))
        gain = gain * jnp.repeat(jnp.exp(steps), dims[position] // shards_of).reshape((-1,) + (1,) * (len(dims) - 1 - position))
    return gain


def bell_draw(rng, dims, scale, limit, split=(), kind=jnp.bfloat16):
    loudness = block_levels(rng, dims, split, -0.22, 0.18) if split else 1.0
    entries = jax.random.normal(rng, dims, jnp.float32) * scale * loudness
    return jnp.minimum(jnp.maximum(entries, -limit), limit).astype(kind)


def setup_inputs(seed: int = 0) -> dict:
    key_list = jax.random.split(jax.random.key(seed), 4)
    return {
        "snapshots": bell_draw(key_list[0], (S, NZ, NY, NXF), 1.0, 6.0, ((1, 64), (2, 2)), jnp.float32),
        "energies": jnp.clip(jnp.exp(jax.random.uniform(key_list[1], (S,), jnp.float32, math.log(0.3), math.log(3.0))), 0.3, 3.0),
        "plane_weight": jnp.clip(jnp.exp(math.log(10.0) - 2.3025851 * jax.random.uniform(key_list[2], (NZ,), jnp.float32) ** block_levels(key_list[2], (NZ,), ((0, 64),), -0.2, 0.2)), 1.0, 10.0),
    }


def reference(snapshots, energies, plane_weight):
    scaled = snapshots * energies[:, None, None, None]
    filtered = 0.25 * jnp.roll(scaled, 1, axis=1) + 0.5 * scaled + 0.25 * jnp.roll(scaled, -1, axis=1)
    total = filtered.shape[1] * filtered.shape[2] * filtered.shape[3]

    def add_plane(index, gram):
        plane = lax.dynamic_index_in_dim(filtered, index, 1, keepdims=False).reshape(S, -1)
        weight = lax.dynamic_index_in_dim(plane_weight, index, 0, keepdims=False)
        return gram + jnp.dot(plane * weight, plane.T, precision=lax.Precision.HIGHEST)
    gram = lax.fori_loop(0, NZ, add_plane, jnp.zeros((S, S), jnp.float32)) / total
    basis = jnp.eye(S, dtype=jnp.float32)[:, :MODES]
    for step in range(ITERS):
        image = jnp.dot(gram, basis, precision=lax.Precision.HIGHEST)
        factor = jnp.linalg.cholesky(jnp.dot(image.T, image, precision=lax.Precision.HIGHEST))
        basis = jax.scipy.linalg.solve_triangular(factor, image.T, lower=True).T
    raw = jnp.dot(basis.T, filtered.reshape(S, -1), precision=lax.Precision.HIGHEST)
    raw = raw.reshape(MODES, NZ, NY, NXF)
    norms = lax.optimization_barrier(jnp.sum(raw * raw * plane_weight[None, :, None, None], axis=(1, 2, 3))) / total
    modes = raw / jnp.sqrt(norms)[:, None, None, None]
    return (modes, basis)
```

```python
import functools

import jax
import jax.numpy as jnp
from jax import lax
from jax.experimental import pallas as pl
from jax.experimental.pallas import tpu as pltpu
from jax.sharding import Mesh
from jax.sharding import PartitionSpec as P

MODES = 16
ITERS = 6
NAMES = ("gz_y", "gz_x", "gz_h", "gz_c", "gy")
GZ = NAMES[:4]
MESH = pl.DeviceIdType.MESH
HIGH = lax.Precision.HIGHEST
F32 = jnp.float32
BF16 = jnp.bfloat16
ROWS = 8


def nt(a, b, precision=None):
    return lax.dot_general(
        a, b, (((1,), (1,)), ((), ())), precision=precision, preferred_element_type=F32
    )


def line_device(index):
    return {"gz_h": index // 4, "gz_c": (index // 2) % 2, "gy": index % 2}


def plane_device(index):
    return {"gz_y": index // 4, "gz_x": index % 4}


def slab_device(index):
    return {
        "gz_y": index // 16,
        "gz_x": (index // 4) % 4,
        "gz_h": (index // 2) % 2,
        "gz_c": index % 2,
    }


def split(x):
    high = x.astype(BF16)
    return high, (x - high.astype(F32)).astype(BF16)


def gram_kernel(
    chunks,
    snap,
    weight,
    filt_out,
    gram_out,
    field,
    below,
    above,
    filt,
    total,
    weights,
    line_buf,
    plane_buf,
    load_sem,
    small_sem,
    store_sem,
    halo_send,
    halo_recv,
    line_send,
    line_recv,
    plane_send,
    plane_recv,
):
    count = field.shape[2]
    tall = count * ROWS
    y, x, h, c, g = (lax.axis_index(name) for name in NAMES)
    slab = ((y * 4 + x) * 2 + h) * 2 + c
    slabs = 64
    upper = slab_device(lax.rem(slab + 1, slabs))
    lower = slab_device(lax.rem(slab + slabs - 1, slabs))
    line = (h * 2 + c) * 2 + g
    plane = y * 4 + x

    barrier = pltpu.get_barrier_semaphore()
    for device in (upper, lower):
        pl.semaphore_signal(barrier, inc=1, device_id=device, device_id_type=MESH)
    for step in range(1, 8):
        device = line_device(lax.rem(line + step, 8))
        pl.semaphore_signal(barrier, inc=1, device_id=device, device_id_type=MESH)
    for step in range(1, 16):
        device = plane_device(lax.rem(plane + step, 16))
        pl.semaphore_signal(barrier, inc=1, device_id=device, device_id_type=MESH)

    def load(chunk, z):
        rows = pl.ds(pl.multiple_of(chunk * ROWS, ROWS), ROWS)
        return pltpu.make_async_copy(
            snap.at[:, z, rows, :], field.at[chunk, z], load_sem.at[chunk, z]
        )

    def halo(chunk, side):
        rows = pl.ds(pl.multiple_of(chunk * ROWS, ROWS), ROWS)
        return pltpu.make_async_remote_copy(
            src_ref=snap.at[:, 3 if side == 0 else 0, rows, :],
            dst_ref=(below if side == 0 else above).at[chunk],
            send_sem=halo_send.at[side, chunk],
            recv_sem=halo_recv.at[side, chunk],
            device_id=upper if side == 0 else lower,
            device_id_type=MESH,
        )

    def store(chunk, z):
        return pltpu.make_async_copy(
            filt.at[z, chunk], filt_out.at[z, chunk], store_sem.at[chunk, z]
        )

    pl.semaphore_wait(barrier, 24)
    for chunk in range(chunks):
        for side in range(2):
            halo(chunk, side).start()
    read = pltpu.make_async_copy(weight, weights, small_sem)
    read.start()
    for chunk in range(chunks):
        for z in range(4):
            load(chunk, z).start()
    read.wait()
    root = [jnp.sqrt(jnp.full((1, 256), weights[z], F32)) for z in range(4)]
    total[...] = jnp.zeros_like(total)

    def smooth(a, b, c, z):
        value = (0.25 * root[z]) * (a + c) + (0.5 * root[z]) * b
        return value

    def accumulate(chunk, planes, values):
        highs, lows = [], []
        for z, value in zip(planes, values):
            high, low = split(value)
            filt[z, chunk, :tall, :] = high
            filt[z, chunk, tall:, :] = low
            highs.append(high)
            lows.append(low)
        high = jnp.concatenate(highs, axis=1)
        low = jnp.concatenate(lows, axis=1)
        total[:, :tall] += nt(high, high)
        total[:, tall:] += nt(high, low)
        for z in planes:
            store(chunk, z).start()

    def flat(ref):
        return ref[...].reshape(tall, ref.shape[-1])

    def inner(chunk, carry):
        for z in range(4):
            load(chunk, z).wait()
        s = [flat(field.at[chunk, z]) for z in range(4)]
        accumulate(
            chunk, (1, 2), [smooth(s[0], s[1], s[2], 1), smooth(s[1], s[2], s[3], 2)]
        )
        return carry

    lax.fori_loop(0, chunks, inner, 0)

    def outer(chunk, carry):
        for side in range(2):
            halo(chunk, side).wait_recv()
        first = smooth(
            flat(below.at[chunk]), flat(field.at[chunk, 0]), flat(field.at[chunk, 1]), 0
        )
        last = smooth(
            flat(field.at[chunk, 2]), flat(field.at[chunk, 3]), flat(above.at[chunk]), 3
        )
        accumulate(chunk, (0, 3), [first, last])
        return carry

    lax.fori_loop(0, chunks, outer, 0)

    whole = total[:, :tall] + 2.0 * total[:, tall:]
    keep = lax.broadcasted_iota(jnp.int32, (tall, tall), 0) % ROWS == (
        lax.broadcasted_iota(jnp.int32, (tall, tall), 1) % ROWS
    )
    picked = jnp.sum(jnp.where(keep, whole, 0.0).reshape(count, ROWS, tall), axis=1)
    half = count // 2
    wide = jnp.concatenate([picked[:half], picked[half:]], axis=1)
    place = lax.broadcasted_iota(jnp.int32, (128, 2 * tall), 1) // ROWS
    place = jnp.where(place < count, place, place - count + 64)
    choose = (place == lax.broadcasted_iota(jnp.int32, (128, 2 * tall), 0)).astype(F32)
    packed = nt(wide, choose, HIGH)

    def reduce(value, buf, me, size, device_of, send, recv):
        buf[me] = value
        copies = []
        for step in range(1, size):
            other = lax.rem(me + step, size)
            copies.append(
                pltpu.make_async_remote_copy(
                    src_ref=buf.at[me],
                    dst_ref=buf.at[me],
                    send_sem=send.at[other],
                    recv_sem=recv.at[me],
                    device_id=device_of(other),
                    device_id_type=MESH,
                )
            )
        for copy in copies:
            copy.start()
        for step in range(1, size):
            other = lax.rem(me + step, size)
            pltpu.make_async_remote_copy(
                src_ref=buf.at[other],
                dst_ref=buf.at[other],
                send_sem=send.at[other],
                recv_sem=recv.at[other],
                device_id=device_of(other),
                device_id_type=MESH,
            ).wait_recv()
        parts = [buf[i] for i in range(size)]
        while len(parts) > 1:
            parts = [parts[i] + parts[i + 1] for i in range(0, len(parts), 2)]
        return parts[0], copies

    packed, line_copies = reduce(
        packed, line_buf, line, 8, line_device, line_send, line_recv
    )
    packed, plane_copies = reduce(
        packed, plane_buf, plane, 16, plane_device, plane_send, plane_recv
    )
    gram_out[...] = packed
    for copy in line_copies + plane_copies:
        copy.wait_send()
    for chunk in range(chunks):
        for side in range(2):
            halo(chunk, side).wait_send()
        for z in range(4):
            store(chunk, z).wait()


def mode_kernel(
    chunks,
    cells,
    packed,
    energy_row,
    energy_col,
    weight,
    filt_in,
    modes_out,
    basis_out,
    filt,
    modes,
    columns,
    lines,
    load_sem,
    store_sem,
):
    count = energy_row.shape[1]
    tall = count * ROWS

    def load(chunk, z):
        return pltpu.make_async_copy(
            filt_in.at[z, chunk], filt.at[z, chunk], load_sem.at[z, chunk]
        )

    def store(chunk, z):
        rows = pl.ds(pl.multiple_of(chunk * ROWS, ROWS), ROWS)
        return pltpu.make_async_copy(
            modes.at[z, chunk], modes_out.at[:, z, rows, :], store_sem.at[z, chunk]
        )

    for z in range(4):
        for chunk in range(chunks):
            load(chunk, z).start()

    half = count // 2
    value = packed[...]
    gram = jnp.concatenate([value[:, :count], value[:, 64 : 64 + count]], axis=0)
    gram = 0.5 * (gram + gram.T)
    gram = gram * (energy_col[...] * energy_row[...]) / cells

    eye = (
        lax.broadcasted_iota(jnp.int32, (MODES, count), 0)
        == lax.broadcasted_iota(jnp.int32, (MODES, count), 1)
    ).astype(F32)

    def iterate(step, basis):
        image = jnp.dot(basis, gram, precision=HIGH, preferred_element_type=F32)
        square = nt(image, image, HIGH)
        for j in range(MODES):
            columns[j] = jnp.broadcast_to(square[:, j : j + 1], (MODES, 128))
        lines[:, :count] = image
        entry = {
            (i, j): columns[j, i : i + 1, :] for j in range(MODES) for i in range(j, MODES)
        }
        row = [lines[i : i + 1, :] for i in range(MODES)]
        for k in range(MODES):
            scale = lax.rsqrt(entry[k, k])
            inverse = scale * scale
            row[k] = row[k]
            factors = {i: entry[i, k] * inverse for i in range(k + 1, MODES)}
            for i in range(k + 1, MODES):
                row[i] = row[i] - factors[i] * row[k]
                for j in range(k + 1, i + 1):
                    entry[i, j] = entry[i, j] - factors[i] * entry[j, k]
            row[k] = row[k] * scale
        for i in range(MODES):
            lines[i : i + 1, :] = row[i]
        return lines[:, :count]

    lines[...] = jnp.zeros_like(lines)
    basis = lax.fori_loop(0, ITERS, iterate, eye)
    basis_out[...] = basis.T
    projected = jnp.dot(basis, gram, precision=HIGH, preferred_element_type=F32)
    norms = jnp.sum(basis * projected, axis=1, keepdims=True)
    scaled = basis * energy_row[...] * lax.rsqrt(norms)
    high, low = split(scaled)
    both = jnp.concatenate([high.astype(F32), low.astype(F32)], axis=0).astype(BF16)
    spread = (
        lax.broadcasted_iota(jnp.int32, (count, tall), 0)
        == lax.broadcasted_iota(jnp.int32, (count, tall), 1) // ROWS
    ).astype(BF16)
    both = jnp.dot(both, spread, preferred_element_type=F32).astype(BF16)
    tallest = 2 * MODES * ROWS
    repeat = (
        lax.broadcasted_iota(jnp.int32, (tallest, 2 * MODES), 0) // ROWS
        == lax.broadcasted_iota(jnp.int32, (tallest, 2 * MODES), 1)
    ).astype(BF16)
    both = jnp.dot(repeat, both, preferred_element_type=F32)
    keep = lax.broadcasted_iota(jnp.int32, (tallest, tall), 0) % ROWS == (
        lax.broadcasted_iota(jnp.int32, (tallest, tall), 1) % ROWS
    )
    both = jnp.where(keep, both, 0.0).astype(BF16)
    top, bottom = both[: MODES * ROWS], both[MODES * ROWS :]

    for z in range(4):
        back = lax.rsqrt(jnp.full((1, 256), weight[z], F32))

        def project(chunk, carry, z=z, back=back):
            load(chunk, z).wait()
            high = filt[z, chunk, :tall, :]
            low = filt[z, chunk, tall:, :]
            raw = jnp.dot(top, high, preferred_element_type=F32)
            raw += jnp.dot(top, low, preferred_element_type=F32)
            raw += jnp.dot(bottom, high, preferred_element_type=F32)
            modes[z, chunk] = (raw * back).reshape(MODES, ROWS, raw.shape[-1])
            store(chunk, z).start()
            return carry

        lax.fori_loop(0, chunks, project, 0)
    for z in range(4):
        for chunk in range(chunks):
            store(chunk, z).wait()


def local(snapshots, energies, plane_weight):
    count, planes, rows, width = snapshots.shape
    chunks = rows // ROWS
    tall = count * ROWS
    any_space = pl.BlockSpec(memory_space=pl.ANY)
    vmem = pl.BlockSpec(memory_space=pltpu.VMEM)
    smem = pl.BlockSpec(memory_space=pltpu.SMEM)
    dma = pltpu.SemaphoreType.DMA
    filt_shape = (planes, chunks, 2 * tall, width)
    filt, packed = pl.pallas_call(
        functools.partial(gram_kernel, chunks),
        name="gram",
        out_shape=(
            jax.ShapeDtypeStruct(filt_shape, BF16),
            jax.ShapeDtypeStruct((count // 2, 128), F32),
        ),
        in_specs=[any_space, any_space],
        out_specs=(any_space, vmem),
        scratch_shapes=[
            pltpu.VMEM((chunks, planes, count, ROWS, width), F32),
            pltpu.VMEM((chunks, count, ROWS, width), F32),
            pltpu.VMEM((chunks, count, ROWS, width), F32),
            pltpu.VMEM(filt_shape, BF16),
            pltpu.VMEM((tall, 2 * tall), F32),
            pltpu.SMEM((planes,), F32),
            pltpu.VMEM((8, count // 2, 128), F32),
            pltpu.VMEM((16, count // 2, 128), F32),
            dma((chunks, planes)),
            dma,
            dma((chunks, planes)),
            dma((2, chunks)),
            dma((2, chunks)),
            dma((8,)),
            dma((8,)),
            dma((16,)),
            dma((16,)),
        ],
        compiler_params=pltpu.CompilerParams(
            collective_id=0, has_side_effects=True, vmem_limit_bytes=60 * 2**20
        ),
    )(snapshots, plane_weight)
    cells = planes * 64 * rows * 2 * width
    modes, basis = pl.pallas_call(
        functools.partial(mode_kernel, chunks, cells),
        name="modes",
        out_shape=(
            jax.ShapeDtypeStruct((MODES, planes, rows, width), F32),
            jax.ShapeDtypeStruct((count, MODES), F32),
        ),
        in_specs=[vmem, vmem, vmem, smem, any_space],
        out_specs=(any_space, vmem),
        scratch_shapes=[
            pltpu.VMEM(filt_shape, BF16),
            pltpu.VMEM((planes, chunks, MODES, ROWS, width), F32),
            pltpu.VMEM((MODES, MODES, 128), F32),
            pltpu.VMEM((MODES, 128), F32),
            dma((planes, chunks)),
            dma((planes, chunks)),
        ],
        compiler_params=pltpu.CompilerParams(vmem_limit_bytes=60 * 2**20),
    )(packed, energies[None, :], energies[:, None], plane_weight, filt)
    return modes, basis


def solution(mesh):
    torus = Mesh(mesh.devices.reshape(4, 4, 2, 2, mesh.shape["gy"]), NAMES)
    in_specs = (P(None, GZ, "gy", None), P(), P(GZ))
    out_specs = (P(None, GZ, "gy", None), P())
    return jax.shard_map(local, mesh=torus, in_specs=in_specs, out_specs=out_specs, check_vma=False)
```

```python
import functools

import jax
import jax.numpy as jnp
from jax import lax
from jax.experimental import pallas as pl
from jax.experimental.pallas import tpu as pltpu
from jax.sharding import Mesh
from jax.sharding import PartitionSpec as P

MODES = 16
ITERS = 6
NAMES = ("gz_y", "gz_x", "gz_h", "gz_c", "gy")
GZ = NAMES[:4]
MESH = pl.DeviceIdType.MESH
HIGH = lax.Precision.HIGHEST
F32 = jnp.float32
BF16 = jnp.bfloat16
ROWS = 8
GROUP = 4
VMEM_GRAM = 40 * 2**20
VMEM_MODES = 24 * 2**20


def nt(a, b, precision=None):
    return lax.dot_general(
        a, b, (((1,), (1,)), ((), ())), precision=precision, preferred_element_type=F32
    )


def line_device(index):
    return {"gz_h": index // 4, "gz_c": (index // 2) % 2, "gy": index % 2}


def plane_device(index):
    return {"gz_y": index // 4, "gz_x": index % 4}


def slab_device(index):
    return {
        "gz_y": index // 16,
        "gz_x": (index // 4) % 4,
        "gz_h": (index // 2) % 2,
        "gz_c": index % 2,
    }


def split(x):
    high = x.astype(BF16)
    return high, (x - high.astype(F32)).astype(BF16)


def gram_kernel(
    chunks,
    snap,
    weight,
    filt,
    gram_out,
    field,
    halos,
    total,
    choose,
    weights,
    line_buf,
    plane_buf,
    load_sem,
    small_sem,
    halo_send,
    halo_recv,
    line_send,
    line_recv,
    plane_send,
    plane_recv,
):
    count = field.shape[2]
    tall = count * ROWS
    y, x, h, c, g = (lax.axis_index(name) for name in NAMES)
    slab = ((y * 4 + x) * 2 + h) * 2 + c
    slabs = 64
    upper = slab_device(lax.rem(slab + 1, slabs))
    lower = slab_device(lax.rem(slab + slabs - 1, slabs))
    line = (h * 2 + c) * 2 + g
    plane = y * 4 + x

    barrier = pltpu.get_barrier_semaphore()
    for device in (upper, lower):
        pl.semaphore_signal(barrier, inc=1, device_id=device, device_id_type=MESH)
    for step in range(1, 8):
        device = line_device(lax.rem(line + step, 8))
        pl.semaphore_signal(barrier, inc=1, device_id=device, device_id_type=MESH)
    for step in range(1, 16):
        device = plane_device(lax.rem(plane + step, 16))
        pl.semaphore_signal(barrier, inc=1, device_id=device, device_id_type=MESH)

    def load(chunk, z):
        rows = pl.ds(pl.multiple_of(chunk * ROWS, ROWS), ROWS)
        return pltpu.make_async_copy(
            snap.at[:, z, rows, :], field.at[chunk, z], load_sem.at[chunk, z]
        )

    def halo(chunk, side):
        rows = pl.ds(pl.multiple_of(chunk * ROWS, ROWS), ROWS)
        return pltpu.make_async_remote_copy(
            src_ref=snap.at[:, 3 if side == 0 else 0, rows, :],
            dst_ref=halos.at[side, chunk],
            send_sem=halo_send.at[side, chunk],
            recv_sem=halo_recv.at[side, chunk],
            device_id=upper if side == 0 else lower,
            device_id_type=MESH,
        )

    def arrival(chunk, side):
        return pltpu.make_async_remote_copy(
            src_ref=halos.at[side, chunk],
            dst_ref=halos.at[side, chunk],
            send_sem=halo_send.at[side, chunk],
            recv_sem=halo_recv.at[side, chunk],
            device_id=upper,
            device_id_type=MESH,
        )

    pl.semaphore_wait(barrier, 24)
    for chunk in range(chunks):
        for side in range(2):
            halo(chunk, side).start()
    read = pltpu.make_async_copy(weight, weights, small_sem)
    read.start()
    for chunk in range(chunks):
        for z in range(4):
            load(chunk, z).start()
    read.wait()
    total[...] = jnp.zeros_like(total)
    place = lax.broadcasted_iota(jnp.int32, (2 * tall, 128), 0) // ROWS
    place = jnp.where(place < count, place, place - count + 64)
    choose[...] = (
        (place == lax.broadcasted_iota(jnp.int32, (2 * tall, 128), 1)).astype(F32).astype(BF16)
    )

    def smooth(a, b, c, z):
        root = jnp.sqrt(jnp.full((1, 256), weights[z], F32))
        return (0.25 * root) * (a + c) + (0.5 * root) * b

    def accumulate(chunk, planes, values):
        highs, lows = [], []
        for z, value in zip(planes, values):
            high, low = split(value)
            filt[z, chunk, :tall, :] = high
            filt[z, chunk, tall:, :] = low
            highs.append(high)
            lows.append(low)
        high = jnp.concatenate(highs, axis=1)
        low = jnp.concatenate(lows, axis=1)
        total[...] += nt(high, jnp.concatenate([high, low], axis=0))

    def flat(ref):
        return ref[...].reshape(tall, ref.shape[-1])

    def inner(chunk, carry):
        for z in range(4):
            load(chunk, z).wait()
        s = [flat(field.at[chunk, z]) for z in range(4)]
        accumulate(
            chunk, (1, 2), [smooth(s[0], s[1], s[2], 1), smooth(s[1], s[2], s[3], 2)]
        )
        return carry

    lax.fori_loop(0, chunks, inner, 0)

    for side in (1 - c, c * 1):
        z = side * 3

        def outer(chunk, carry, side=side, z=z):
            arrival(chunk, side).wait_recv()
            value = smooth(
                flat(halos.at[side, chunk]),
                flat(field.at[chunk, z]),
                flat(field.at[chunk, 1 + side]),
                z,
            )
            accumulate(chunk, (z,), [value])
            return carry

        lax.fori_loop(0, chunks, outer, 0)

    whole = total[:, :tall] + 2.0 * total[:, tall:]
    keep = lax.broadcasted_iota(jnp.int32, (tall, tall), 0) % ROWS == (
        lax.broadcasted_iota(jnp.int32, (tall, tall), 1) % ROWS
    )
    picked = jnp.sum(jnp.where(keep, whole, 0.0).reshape(count, ROWS, tall), axis=1)
    half = count // 2
    wide = jnp.concatenate([picked[:half], picked[half:]], axis=1)
    packed = jnp.zeros((half, 128), F32)
    rest = wide
    for part in range(3):
        piece = rest.astype(BF16)
        rest = rest - piece.astype(F32)
        packed += jnp.dot(piece, choose[...], preferred_element_type=F32)

    def reduce(value, buf, me, size, device_of, send, recv):
        buf[me] = value
        copies = []
        for step in range(1, size):
            other = lax.rem(me + step, size)
            copies.append(
                pltpu.make_async_remote_copy(
                    src_ref=buf.at[me],
                    dst_ref=buf.at[me],
                    send_sem=send.at[other],
                    recv_sem=recv.at[me],
                    device_id=device_of(other),
                    device_id_type=MESH,
                )
            )
        for copy in copies:
            copy.start()
        for step in range(1, size):
            other = lax.rem(me + step, size)
            pltpu.make_async_remote_copy(
                src_ref=buf.at[other],
                dst_ref=buf.at[other],
                send_sem=send.at[other],
                recv_sem=recv.at[other],
                device_id=device_of(other),
                device_id_type=MESH,
            ).wait_recv()
        parts = [buf[i] for i in range(size)]
        while len(parts) > 1:
            parts = [parts[i] + parts[i + 1] for i in range(0, len(parts), 2)]
        return parts[0], copies

    packed, line_copies = reduce(
        packed, line_buf, line, 8, line_device, line_send, line_recv
    )
    packed, plane_copies = reduce(
        packed, plane_buf, plane, 16, plane_device, plane_send, plane_recv
    )
    gram_out[...] = packed
    for copy in line_copies + plane_copies:
        copy.wait_send()
    for chunk in range(chunks):
        for side in range(2):
            halo(chunk, side).wait_send()


def mode_kernel(
    chunks,
    cells,
    packed,
    energy_row,
    weight,
    filt,
    modes_out,
    basis_out,
    modes,
    columns,
    lines,
    store_sem,
):
    count = energy_row.shape[1]
    tall = count * ROWS

    def store(chunk, z):
        rows = pl.ds(pl.multiple_of(chunk * ROWS, ROWS), ROWS)
        return pltpu.make_async_copy(
            modes.at[z, chunk], modes_out.at[:, z, rows, :], store_sem.at[z, chunk]
        )

    half = count // 2
    value = packed[...]
    gram = jnp.concatenate([value[:, :count], value[:, 64 : 64 + count]], axis=0)
    gram = (gram * energy_row[...]).T * energy_row[...]
    gram = (0.5 / cells) * (gram + gram.T)

    eye = (
        lax.broadcasted_iota(jnp.int32, (MODES, count), 0)
        == lax.broadcasted_iota(jnp.int32, (MODES, count), 1)
    ).astype(F32)

    def iterate(step, basis):
        image = jnp.dot(basis, gram, precision=HIGH, preferred_element_type=F32)
        square = nt(image, image, HIGH)
        for j in range(MODES):
            columns[j] = jnp.broadcast_to(square[:, j : j + 1], (MODES, 128))
        lines[:, :count] = image
        entry = {
            (i, j): columns[j, i : i + 1, :] for j in range(MODES) for i in range(j, MODES)
        }
        row = [lines[i : i + 1, :] for i in range(MODES)]
        for k in range(MODES):
            scale = lax.rsqrt(entry[k, k])
            inverse = scale * scale
            factors = {i: entry[i, k] * inverse for i in range(k + 1, MODES)}
            for i in range(k + 1, MODES):
                row[i] = row[i] - factors[i] * row[k]
                for j in range(k + 1, i + 1):
                    entry[i, j] = entry[i, j] - factors[i] * entry[j, k]
            row[k] = row[k] * scale
        for i in range(MODES):
            lines[i : i + 1, :] = row[i]
        return lines[:, :count]

    lines[...] = jnp.zeros_like(lines)
    basis = lax.fori_loop(0, ITERS, iterate, eye)
    basis_out[...] = basis
    projected = jnp.dot(basis, gram, precision=HIGH, preferred_element_type=F32)
    norms = jnp.sum(basis * projected, axis=1, keepdims=True)
    scaled = basis * energy_row[...] * lax.rsqrt(norms)
    high, low = split(scaled)
    both = jnp.concatenate([high.astype(F32), low.astype(F32)], axis=0).astype(BF16)
    spread = (
        lax.broadcasted_iota(jnp.int32, (count, tall), 0)
        == lax.broadcasted_iota(jnp.int32, (count, tall), 1) // ROWS
    ).astype(F32).astype(BF16)
    both = jnp.dot(both, spread, preferred_element_type=F32)
    both = jnp.broadcast_to(both[:, None, :], (2 * MODES, ROWS, tall))
    keep = lax.broadcasted_iota(jnp.int32, both.shape, 1) == (
        lax.broadcasted_iota(jnp.int32, both.shape, 2) % ROWS
    )
    both = jnp.where(keep, both, 0.0).reshape(2 * MODES * ROWS, tall).astype(BF16)
    top, bottom = both[: MODES * ROWS], both[MODES * ROWS :]
    matrix = jnp.concatenate([top, top, bottom], axis=1)

    def project(step, carry):
        z = step // (chunks // GROUP)
        first = lax.rem(step, chunks // GROUP) * GROUP
        back = lax.rsqrt(jnp.full((1, modes.shape[-1]), weight[z], F32))
        fields = []
        for i in range(GROUP):
            value = filt[z, first + i]
            fields.append(jnp.concatenate([value, value[:tall]], axis=0))
        raw = jnp.dot(
            matrix, jnp.concatenate(fields, axis=1), preferred_element_type=F32
        )
        width = modes.shape[-1]
        for i in range(GROUP):
            part = raw[:, i * width : (i + 1) * width] * back
            modes[z, first + i] = part.reshape(MODES, ROWS, width)
            store(first + i, z).start()
        return carry

    lax.fori_loop(0, 4 * chunks // GROUP, project, 0)
    for z in range(4):
        for chunk in range(chunks):
            store(chunk, z).wait()


def local(snapshots, energies, plane_weight):
    count, planes, rows, width = snapshots.shape
    chunks = rows // ROWS
    tall = count * ROWS
    any_space = pl.BlockSpec(memory_space=pl.ANY)
    hbm = pl.BlockSpec(memory_space=pltpu.HBM)
    vmem = pl.BlockSpec(memory_space=pltpu.VMEM)
    smem = pl.BlockSpec(memory_space=pltpu.SMEM)
    dma = pltpu.SemaphoreType.DMA
    filt_shape = (planes, chunks, 2 * tall, width)
    filt, packed = pl.pallas_call(
        functools.partial(gram_kernel, chunks),
        name="gram",
        out_shape=(
            pltpu.VMEM(filt_shape, BF16),
            pltpu.VMEM((count // 2, 128), F32),
        ),
        in_specs=[hbm, hbm],
        out_specs=(vmem, vmem),
        scratch_shapes=[
            pltpu.VMEM((chunks, planes, count, ROWS, width), F32),
            pltpu.VMEM((2, chunks, count, ROWS, width), F32),
            pltpu.VMEM((tall, 2 * tall), F32),
            pltpu.VMEM((2 * tall, 128), BF16),
            pltpu.SMEM((planes,), F32),
            pltpu.VMEM((8, count // 2, 128), F32),
            pltpu.VMEM((16, count // 2, 128), F32),
            dma((chunks, planes)),
            dma,
            dma((2, chunks)),
            dma((2, chunks)),
            dma((8,)),
            dma((8,)),
            dma((16,)),
            dma((16,)),
        ],
        compiler_params=pltpu.CompilerParams(
            collective_id=0, has_side_effects=True, vmem_limit_bytes=VMEM_GRAM
        ),
    )(
        pltpu.with_memory_space_constraint(snapshots, pltpu.HBM),
        pltpu.with_memory_space_constraint(plane_weight, pltpu.HBM),
    )
    cells = planes * 64 * rows * 2 * width
    modes, basis = pl.pallas_call(
        functools.partial(mode_kernel, chunks, cells),
        name="modes",
        out_shape=(
            jax.ShapeDtypeStruct((MODES, planes, rows, width), F32),
            jax.ShapeDtypeStruct((MODES, count), F32),
        ),
        in_specs=[vmem, vmem, smem, vmem],
        out_specs=(any_space, vmem),
        scratch_shapes=[
            pltpu.VMEM((planes, chunks, MODES, ROWS, width), F32),
            pltpu.VMEM((MODES, MODES, 128), F32),
            pltpu.VMEM((MODES, 128), F32),
            dma((planes, chunks)),
        ],
        compiler_params=pltpu.CompilerParams(vmem_limit_bytes=VMEM_MODES),
    )(
        pltpu.with_memory_space_constraint(packed, pltpu.VMEM),
        energies[None, :],
        plane_weight,
        pltpu.with_memory_space_constraint(filt, pltpu.VMEM),
    )
    return modes, basis.T


def solution(mesh):
    torus = Mesh(mesh.devices.reshape(4, 4, 2, 2, mesh.shape["gy"]), NAMES)
    in_specs = (P(None, GZ, "gy", None), P(), P(GZ))
    out_specs = (P(None, GZ, "gy", None), P())
    return jax.shard_map(local, mesh=torus, in_specs=in_specs, out_specs=out_specs, check_vma=False)
```

```python
import functools

import jax
import jax.numpy as jnp
from jax import lax
from jax.experimental import pallas as pl
from jax.experimental.pallas import tpu as pltpu
from jax.sharding import Mesh
from jax.sharding import PartitionSpec as P

MODES = 16
ITERS = 6
NAMES = ("gz_y", "gz_x", "gz_h", "gz_c", "gy")
GZ = NAMES[:4]
MESH = pl.DeviceIdType.MESH
HIGH = lax.Precision.HIGHEST
F32 = jnp.float32
BF16 = jnp.bfloat16
ROWS = 8
GROUP = 4
VMEM_GRAM = 40 * 2**20
VMEM_MODES = 24 * 2**20


def nt(a, b, precision=None):
    return lax.dot_general(
        a, b, (((1,), (1,)), ((), ())), precision=precision, preferred_element_type=F32
    )


def line_device(index):
    return {"gz_h": index // 4, "gz_c": (index // 2) % 2, "gy": index % 2}


def plane_device(index):
    return {"gz_y": index // 4, "gz_x": index % 4}


def slab_device(index):
    return {
        "gz_y": index // 16,
        "gz_x": (index // 4) % 4,
        "gz_h": (index // 2) % 2,
        "gz_c": index % 2,
    }


def split(x):
    high = x.astype(BF16)
    return high, (x - high.astype(F32)).astype(BF16)


def gram_kernel(
    chunks,
    cells,
    snap,
    weight,
    energy_in,
    filt,
    gram_out,
    field,
    halos,
    total,
    choose,
    levels,
    energy_row,
    weights,
    line_buf,
    plane_buf,
    load_sem,
    small_sem,
    energy_sem,
    halo_send,
    halo_recv,
    line_send,
    line_recv,
    plane_send,
    plane_recv,
):
    count = field.shape[2]
    tall = count * ROWS
    y, x, h, c, g = (lax.axis_index(name) for name in NAMES)
    slab = ((y * 4 + x) * 2 + h) * 2 + c
    slabs = 64
    upper = slab_device(lax.rem(slab + 1, slabs))
    lower = slab_device(lax.rem(slab + slabs - 1, slabs))
    line = (h * 2 + c) * 2 + g
    plane = y * 4 + x

    barrier = pltpu.get_barrier_semaphore()
    for device in (upper, lower):
        pl.semaphore_signal(barrier, inc=1, device_id=device, device_id_type=MESH)
    for step in range(1, 8):
        device = line_device(lax.rem(line + step, 8))
        pl.semaphore_signal(barrier, inc=1, device_id=device, device_id_type=MESH)
    for step in range(1, 16):
        device = plane_device(lax.rem(plane + step, 16))
        pl.semaphore_signal(barrier, inc=1, device_id=device, device_id_type=MESH)

    def load(chunk, z):
        rows = pl.ds(pl.multiple_of(chunk * ROWS, ROWS), ROWS)
        return pltpu.make_async_copy(
            snap.at[:, z, rows, :], field.at[chunk, z], load_sem.at[chunk, z]
        )

    def halo(chunk, side):
        rows = pl.ds(pl.multiple_of(chunk * ROWS, ROWS), ROWS)
        return pltpu.make_async_remote_copy(
            src_ref=snap.at[:, 3 if side == 0 else 0, rows, :],
            dst_ref=halos.at[side, chunk],
            send_sem=halo_send.at[side, chunk],
            recv_sem=halo_recv.at[side, chunk],
            device_id=upper if side == 0 else lower,
            device_id_type=MESH,
        )

    def arrival(chunk, side):
        return pltpu.make_async_remote_copy(
            src_ref=halos.at[side, chunk],
            dst_ref=halos.at[side, chunk],
            send_sem=halo_send.at[side, chunk],
            recv_sem=halo_recv.at[side, chunk],
            device_id=upper,
            device_id_type=MESH,
        )

    pl.semaphore_wait(barrier, 24)
    for chunk in range(chunks):
        for side in range(2):
            halo(chunk, side).start()
    read = pltpu.make_async_copy(weight, weights, small_sem)
    read.start()
    fetch = pltpu.make_async_copy(energy_in, energy_row, energy_sem)
    fetch.start()
    for chunk in range(chunks):
        for z in range(4):
            load(chunk, z).start()
    read.wait()
    fetch.wait()
    total[...] = jnp.zeros_like(total)
    place = lax.broadcasted_iota(jnp.int32, (2 * tall, 128), 0) // ROWS
    place = jnp.where(place < count, place, place - count + 64)
    choose[...] = (
        (place == lax.broadcasted_iota(jnp.int32, (2 * tall, 128), 1)).astype(F32).astype(BF16)
    )

    half = count // 2
    pad = jnp.zeros((1, 64 - count), F32)
    energy = energy_row[...]
    across = jnp.concatenate([energy, pad, energy, pad], axis=1)
    down = jnp.broadcast_to(energy, (128, count)).T
    lane = lax.broadcasted_iota(jnp.int32, (half, 128), 1)
    levels[...] = jnp.where(lane < 64, down[:half], down[half:]) * across * (0.5 / cells)

    def smooth(a, b, c, z):
        root = jnp.sqrt(jnp.full((1, 256), weights[z], F32))
        return (0.25 * root) * (a + c) + (0.5 * root) * b

    def accumulate(chunk, planes, values):
        highs, lows = [], []
        for z, value in zip(planes, values):
            high, low = split(value)
            filt[z, chunk, :tall, :] = high
            filt[z, chunk, tall:, :] = low
            highs.append(high)
            lows.append(low)
        high = jnp.concatenate(highs, axis=1)
        low = jnp.concatenate(lows, axis=1)
        total[...] += nt(high, jnp.concatenate([high, low], axis=0))

    def flat(ref):
        return ref[...].reshape(tall, ref.shape[-1])

    def inner(chunk, carry):
        for z in range(4):
            load(chunk, z).wait()
        s = [flat(field.at[chunk, z]) for z in range(4)]
        accumulate(
            chunk, (1, 2), [smooth(s[0], s[1], s[2], 1), smooth(s[1], s[2], s[3], 2)]
        )
        return carry

    lax.fori_loop(0, chunks, inner, 0)

    for side in (1 - c, c * 1):
        z = side * 3

        def outer(chunk, carry, side=side, z=z):
            arrival(chunk, side).wait_recv()
            value = smooth(
                flat(halos.at[side, chunk]),
                flat(field.at[chunk, z]),
                flat(field.at[chunk, 1 + side]),
                z,
            )
            accumulate(chunk, (z,), [value])
            return carry

        lax.fori_loop(0, chunks, outer, 0)

    whole = total[:, :tall] + 2.0 * total[:, tall:]
    keep = lax.broadcasted_iota(jnp.int32, (tall, tall), 0) % ROWS == (
        lax.broadcasted_iota(jnp.int32, (tall, tall), 1) % ROWS
    )
    picked = jnp.sum(jnp.where(keep, whole, 0.0).reshape(count, ROWS, tall), axis=1)
    wide = jnp.concatenate([picked[:half], picked[half:]], axis=1)
    packed = jnp.zeros((half, 128), F32)
    rest = wide
    for part in range(3):
        piece = rest.astype(BF16)
        rest = rest - piece.astype(F32)
        packed += jnp.dot(piece, choose[...], preferred_element_type=F32)

    def reduce(value, buf, me, size, device_of, send, recv):
        buf[me] = value
        copies = []
        for step in range(1, size):
            other = lax.rem(me + step, size)
            copies.append(
                pltpu.make_async_remote_copy(
                    src_ref=buf.at[me],
                    dst_ref=buf.at[me],
                    send_sem=send.at[other],
                    recv_sem=recv.at[me],
                    device_id=device_of(other),
                    device_id_type=MESH,
                )
            )
        for copy in copies:
            copy.start()
        for step in range(1, size):
            other = lax.rem(me + step, size)
            pltpu.make_async_remote_copy(
                src_ref=buf.at[other],
                dst_ref=buf.at[other],
                send_sem=send.at[other],
                recv_sem=recv.at[other],
                device_id=device_of(other),
                device_id_type=MESH,
            ).wait_recv()
        parts = [buf[i] for i in range(size)]
        while len(parts) > 1:
            parts = [parts[i] + parts[i + 1] for i in range(0, len(parts), 2)]
        return parts[0], copies

    packed, line_copies = reduce(
        packed, line_buf, line, 8, line_device, line_send, line_recv
    )
    packed, plane_copies = reduce(
        packed, plane_buf, plane, 16, plane_device, plane_send, plane_recv
    )
    gram_out[...] = packed * levels[...]
    for copy in line_copies + plane_copies:
        copy.wait_send()
    for chunk in range(chunks):
        for side in range(2):
            halo(chunk, side).wait_send()


def mode_kernel(
    chunks,
    packed,
    energy_row,
    weight,
    filt,
    modes_out,
    basis_out,
    modes,
    columns,
    lines,
    square_gram,
    store_sem,
):
    count = energy_row.shape[1]
    tall = count * ROWS

    def store(chunk, z):
        rows = pl.ds(pl.multiple_of(chunk * ROWS, ROWS), ROWS)
        return pltpu.make_async_copy(
            modes.at[z, chunk], modes_out.at[:, z, rows, :], store_sem.at[z, chunk]
        )

    square_gram[...] = jnp.zeros_like(square_gram)
    value = packed[...]
    gram = jnp.concatenate([value[:, :count], value[:, 64 : 64 + count]], axis=0)
    square_gram[:count, :count] = gram + gram.T
    gram = square_gram[...]

    def eliminate(image, *arrays):
        square = nt(image, image, HIGH)
        for j in range(MODES):
            columns[j] = jnp.broadcast_to(square[:, j : j + 1], (MODES, 128))
        for i, array in enumerate(arrays):
            lines[i] = array
        entry = {
            (i, j): columns[j, i : i + 1, :] for j in range(MODES) for i in range(j, MODES)
        }
        rows = [[lines[n, i : i + 1, :] for i in range(MODES)] for n in range(len(arrays))]
        for k in range(MODES):
            inverse = 1.0 / entry[k, k]
            if k + 1 < MODES:
                side = entry[k + 1, k]
                entry[k + 1, k + 1] = entry[k + 1, k + 1] - (side * side) * inverse
            for i in range(k + 1, MODES):
                factor = entry[i, k] * inverse
                for row in rows:
                    row[i] = row[i] - factor * row[k]
                for j in range(k + 1, i + 1):
                    if (i, j) != (k + 1, k + 1):
                        entry[i, j] = entry[i, j] - factor * entry[j, k]
            scale = lax.rsqrt(entry[k, k])
            for row in rows:
                row[k] = row[k] * scale
        for n, row in enumerate(rows):
            for i in range(MODES):
                lines[n, i : i + 1, :] = row[i]
        return [lines[n] for n in range(len(arrays))]

    def apply(image):
        return jnp.dot(image, gram, precision=HIGH, preferred_element_type=F32)

    image = lax.fori_loop(
        0, ITERS - 1, lambda step, image: eliminate(image, apply(image))[0], gram[:MODES]
    )
    basis, projected = (x[:, :count] for x in eliminate(image, image, apply(image)))
    basis_out[...] = basis
    norms = jnp.sum(basis * projected, axis=1, keepdims=True)
    scaled = basis * energy_row[...] * lax.rsqrt(norms)
    high, low = split(scaled)
    both = jnp.concatenate([high.astype(F32), low.astype(F32)], axis=0).astype(BF16)
    spread = (
        lax.broadcasted_iota(jnp.int32, (count, tall), 0)
        == lax.broadcasted_iota(jnp.int32, (count, tall), 1) // ROWS
    ).astype(F32).astype(BF16)
    both = jnp.dot(both, spread, preferred_element_type=F32)
    both = jnp.broadcast_to(both[:, None, :], (2 * MODES, ROWS, tall))
    keep = lax.broadcasted_iota(jnp.int32, both.shape, 1) == (
        lax.broadcasted_iota(jnp.int32, both.shape, 2) % ROWS
    )
    both = jnp.where(keep, both, 0.0).reshape(2 * MODES * ROWS, tall).astype(BF16)
    top, bottom = both[: MODES * ROWS], both[MODES * ROWS :]
    matrix = jnp.concatenate([top, top, bottom], axis=1)

    def project(step, carry):
        z = step // (chunks // GROUP)
        first = (step % (chunks // GROUP)) * GROUP
        back = lax.rsqrt(jnp.full((1, modes.shape[-1]), weight[z], F32))
        fields = []
        for i in range(GROUP):
            value = filt[z, first + i]
            fields.append(jnp.concatenate([value, value[:tall]], axis=0))
        raw = jnp.dot(
            matrix, jnp.concatenate(fields, axis=1), preferred_element_type=F32
        )
        width = modes.shape[-1]
        for i in range(GROUP):
            part = raw[:, i * width : (i + 1) * width] * back
            modes[z, first + i] = part.reshape(MODES, ROWS, width)
            store(first + i, z).start()
        return carry

    for step in range(4 * chunks // GROUP):
        project(step, 0)
    for z in range(4):
        for chunk in range(chunks):
            store(chunk, z).wait()


def local(snapshots, energies, plane_weight):
    count, planes, rows, width = snapshots.shape
    chunks = rows // ROWS
    cells = planes * 64 * rows * 2 * width
    tall = count * ROWS
    any_space = pl.BlockSpec(memory_space=pl.ANY)
    hbm = pl.BlockSpec(memory_space=pltpu.HBM)
    vmem = pl.BlockSpec(memory_space=pltpu.VMEM)
    smem = pl.BlockSpec(memory_space=pltpu.SMEM)
    dma = pltpu.SemaphoreType.DMA
    filt_shape = (planes, chunks, 2 * tall, width)
    filt, packed = pl.pallas_call(
        functools.partial(gram_kernel, chunks, cells),
        name="gram",
        out_shape=(
            pltpu.VMEM(filt_shape, BF16),
            pltpu.VMEM((count // 2, 128), F32),
        ),
        in_specs=[hbm, hbm, hbm],
        out_specs=(vmem, vmem),
        scratch_shapes=[
            pltpu.VMEM((chunks, planes, count, ROWS, width), F32),
            pltpu.VMEM((2, chunks, count, ROWS, width), F32),
            pltpu.VMEM((tall, 2 * tall), F32),
            pltpu.VMEM((2 * tall, 128), BF16),
            pltpu.VMEM((count // 2, 128), F32),
            pltpu.VMEM((1, count), F32),
            pltpu.SMEM((planes,), F32),
            pltpu.VMEM((8, count // 2, 128), F32),
            pltpu.VMEM((16, count // 2, 128), F32),
            dma((chunks, planes)),
            dma,
            dma,
            dma((2, chunks)),
            dma((2, chunks)),
            dma((8,)),
            dma((8,)),
            dma((16,)),
            dma((16,)),
        ],
        compiler_params=pltpu.CompilerParams(
            collective_id=0, has_side_effects=True, vmem_limit_bytes=VMEM_GRAM
        ),
    )(
        pltpu.with_memory_space_constraint(snapshots, pltpu.HBM),
        pltpu.with_memory_space_constraint(plane_weight, pltpu.HBM),
        pltpu.with_memory_space_constraint(energies[None, :], pltpu.HBM),
    )
    modes, basis = pl.pallas_call(
        functools.partial(mode_kernel, chunks),
        name="modes",
        out_shape=(
            jax.ShapeDtypeStruct((MODES, planes, rows, width), F32),
            jax.ShapeDtypeStruct((MODES, count), F32),
        ),
        in_specs=[vmem, vmem, smem, vmem],
        out_specs=(any_space, vmem),
        scratch_shapes=[
            pltpu.VMEM((planes, chunks, MODES, ROWS, width), F32),
            pltpu.VMEM((MODES, MODES, 128), F32),
            pltpu.VMEM((2, MODES, 128), F32),
            pltpu.VMEM((128, 128), F32),
            dma((planes, chunks)),
        ],
        compiler_params=pltpu.CompilerParams(vmem_limit_bytes=VMEM_MODES),
    )(
        pltpu.with_memory_space_constraint(packed, pltpu.VMEM),
        energies[None, :],
        plane_weight,
        pltpu.with_memory_space_constraint(filt, pltpu.VMEM),
    )
    return modes, basis.T


def solution(mesh):
    torus = Mesh(mesh.devices.reshape(4, 4, 2, 2, mesh.shape["gy"]), NAMES)
    in_specs = (P(None, GZ, "gy", None), P(), P(GZ))
    out_specs = (P(None, GZ, "gy", None), P())
    return jax.shard_map(local, mesh=torus, in_specs=in_specs, out_specs=out_specs, check_vma=False)
```

```python
import functools

import jax
import jax.numpy as jnp
from jax import lax
from jax.experimental import pallas as pl
from jax.experimental.pallas import tpu as pltpu
from jax.sharding import Mesh
from jax.sharding import PartitionSpec as P

MODES = 16
ITERS = 6
NAMES = ("gz_y", "gz_x", "gz_h", "gz_c", "gy")
GZ = NAMES[:4]
MESH = pl.DeviceIdType.MESH
HIGH = lax.Precision.HIGHEST
F32 = jnp.float32
BF16 = jnp.bfloat16
ROWS = 8
BLOCK = 16
GROUP = 4
VMEM_GRAM = 40 * 2**20
VMEM_MODES = 24 * 2**20


def nt(a, b, precision=None):
    return lax.dot_general(
        a, b, (((1,), (1,)), ((), ())), precision=precision, preferred_element_type=F32
    )


def line_device(index):
    return {"gz_h": index // 4, "gz_c": (index // 2) % 2, "gy": index % 2}


def plane_device(index):
    return {"gz_y": index // 4, "gz_x": index % 4}


def slab_device(index):
    return {
        "gz_y": index // 16,
        "gz_x": (index // 4) % 4,
        "gz_h": (index // 2) % 2,
        "gz_c": index % 2,
    }


def split(x):
    high = x.astype(BF16)
    return high, (x - high.astype(F32)).astype(BF16)


def gram_kernel(
    chunks,
    cells,
    snap,
    weight,
    energy_in,
    filt,
    gram_out,
    field,
    halos,
    total,
    choose,
    levels,
    energy_row,
    weights,
    line_buf,
    plane_buf,
    load_sem,
    small_sem,
    energy_sem,
    halo_send,
    halo_recv,
    line_send,
    line_recv,
    plane_send,
    plane_recv,
):
    count = field.shape[2]
    tall = count * ROWS
    y, x, h, c, g = (lax.axis_index(name) for name in NAMES)
    slab = ((y * 4 + x) * 2 + h) * 2 + c
    slabs = 64
    upper = slab_device(lax.rem(slab + 1, slabs))
    lower = slab_device(lax.rem(slab + slabs - 1, slabs))
    line = (h * 2 + c) * 2 + g
    plane = y * 4 + x

    barrier = pltpu.get_barrier_semaphore()
    for device in (upper, lower):
        pl.semaphore_signal(barrier, inc=1, device_id=device, device_id_type=MESH)
    for step in range(1, 8):
        device = line_device(lax.rem(line + step, 8))
        pl.semaphore_signal(barrier, inc=1, device_id=device, device_id_type=MESH)
    for step in range(1, 16):
        device = plane_device(lax.rem(plane + step, 16))
        pl.semaphore_signal(barrier, inc=1, device_id=device, device_id_type=MESH)

    def load(chunk, z):
        rows = pl.ds(pl.multiple_of(chunk * ROWS, ROWS), ROWS)
        return pltpu.make_async_copy(
            snap.at[:, z, rows, :], field.at[chunk, z], load_sem.at[chunk, z]
        )

    def halo(chunk, side):
        return pltpu.make_async_remote_copy(
            src_ref=field.at[chunk, 3 if side == 0 else 0],
            dst_ref=halos.at[side, chunk],
            send_sem=halo_send.at[side, chunk],
            recv_sem=halo_recv.at[side, chunk],
            device_id=upper if side == 0 else lower,
            device_id_type=MESH,
        )

    def arrival(chunk, side):
        return pltpu.make_async_remote_copy(
            src_ref=halos.at[side, chunk],
            dst_ref=halos.at[side, chunk],
            send_sem=halo_send.at[side, chunk],
            recv_sem=halo_recv.at[side, chunk],
            device_id=upper,
            device_id_type=MESH,
        )

    for chunk in range(chunks):
        for z in (3, 0):
            load(chunk, z).start()
    for chunk in range(chunks):
        for z in (1, 2):
            load(chunk, z).start()
    read = pltpu.make_async_copy(weight, weights, small_sem)
    read.start()
    fetch = pltpu.make_async_copy(energy_in, energy_row, energy_sem)
    fetch.start()
    pl.semaphore_wait(barrier, 24)
    for chunk in range(chunks):
        for side in range(2):
            load(chunk, 3 if side == 0 else 0).wait()
            halo(chunk, side).start()
    read.wait()
    fetch.wait()
    total[...] = jnp.zeros_like(total)
    place = lax.broadcasted_iota(jnp.int32, (3 * tall, 128), 0) // ROWS
    lane = lax.broadcasted_iota(jnp.int32, (3 * tall, 128), 1)
    second, third = place - count, place - 2 * count
    second = jnp.where(second >= BLOCK, second + 2 * BLOCK, -1)
    third = jnp.where(third >= 2 * BLOCK, third + 3 * BLOCK, -1)
    target = jnp.where(place < count, place, jnp.where(place < 2 * count, second, third))
    choose[...] = (target == lane).astype(F32).astype(BF16)

    energy = energy_row[...]
    across = jnp.concatenate(
        [energy, energy[:, BLOCK:], energy[:, 2 * BLOCK :], jnp.zeros((1, 2 * BLOCK), F32)],
        axis=1,
    )
    down = jnp.broadcast_to(energy, (128, count)).T
    lane = lax.broadcasted_iota(jnp.int32, (BLOCK, 128), 1)
    down = jnp.where(
        lane < count,
        down[:BLOCK],
        jnp.where(lane < 2 * count - BLOCK, down[BLOCK : 2 * BLOCK], down[2 * BLOCK :]),
    )
    levels[...] = down * across * (1.0 / cells)

    def smooth(a, b, c, z):
        root = jnp.sqrt(jnp.full((1, 256), weights[z], F32))
        return (0.25 * root) * (a + c) + (0.5 * root) * b

    def accumulate(chunk, planes, values):
        highs, lows = [], []
        for z, value in zip(planes, values):
            high, low = split(value)
            filt[z, chunk, :tall, :] = high
            filt[z, chunk, tall:, :] = low
            highs.append(high)
            lows.append(low)
        high = jnp.concatenate(highs, axis=1)
        low = jnp.concatenate(lows, axis=1)
        total[...] += nt(
            jnp.concatenate([high, high, low], axis=1),
            jnp.concatenate([high, low, high], axis=1),
        )

    def flat(ref):
        return ref[...].reshape(tall, ref.shape[-1])

    def inner(chunk, carry):
        for z in (1, 2):
            load(chunk, z).wait()
        s = [flat(field.at[chunk, z]) for z in range(4)]
        accumulate(
            chunk, (1, 2), [smooth(s[0], s[1], s[2], 1), smooth(s[1], s[2], s[3], 2)]
        )
        return carry

    lax.fori_loop(0, chunks, inner, 0)

    for side in (1 - c, c * 1):
        z = side * 3

        def outer(chunk, carry, side=side, z=z):
            arrival(chunk, side).wait_recv()
            value = smooth(
                flat(halos.at[side, chunk]),
                flat(field.at[chunk, z]),
                flat(field.at[chunk, 1 + side]),
                z,
            )
            accumulate(chunk, (z,), [value])
            return carry

        lax.fori_loop(0, chunks, outer, 0)

    keep = lax.broadcasted_iota(jnp.int32, (tall, tall), 0) % ROWS == (
        lax.broadcasted_iota(jnp.int32, (tall, tall), 1) % ROWS
    )
    picked = jnp.sum(
        jnp.where(keep, total[...], 0.0).reshape(count, ROWS, tall), axis=1
    )
    rest = jnp.concatenate(
        [picked[:BLOCK], picked[BLOCK : 2 * BLOCK], picked[2 * BLOCK :]], axis=1
    )
    pieces = []
    for part in range(3):
        piece = rest.astype(BF16).astype(F32)
        rest = rest - piece
        pieces.append(piece)
    pieces = jnp.concatenate(pieces, axis=0).astype(BF16)
    pieces = jnp.dot(pieces, choose[...], preferred_element_type=F32)
    packed = pieces[:BLOCK] + pieces[BLOCK : 2 * BLOCK] + pieces[2 * BLOCK :]

    def reduce(value, buf, me, size, device_of, send, recv):
        buf[me] = value
        copies = []
        for step in range(1, size):
            other = lax.rem(me + step, size)
            copies.append(
                pltpu.make_async_remote_copy(
                    src_ref=buf.at[me],
                    dst_ref=buf.at[me],
                    send_sem=send.at[other],
                    recv_sem=recv.at[me],
                    device_id=device_of(other),
                    device_id_type=MESH,
                )
            )
        for copy in copies:
            copy.start()
        for step in range(1, size):
            other = lax.rem(me + step, size)
            pltpu.make_async_remote_copy(
                src_ref=buf.at[other],
                dst_ref=buf.at[other],
                send_sem=send.at[other],
                recv_sem=recv.at[other],
                device_id=device_of(other),
                device_id_type=MESH,
            ).wait_recv()
        parts = [buf[i] for i in range(size)]
        while len(parts) > 1:
            parts = [parts[i] + parts[i + 1] for i in range(0, len(parts), 2)]
        return parts[0], copies

    packed, line_copies = reduce(
        packed, line_buf, line, 8, line_device, line_send, line_recv
    )
    packed, plane_copies = reduce(
        packed, plane_buf, plane, 16, plane_device, plane_send, plane_recv
    )
    gram_out[...] = packed * levels[...]
    for copy in line_copies + plane_copies:
        copy.wait_send()
    for chunk in range(chunks):
        for side in range(2):
            halo(chunk, side).wait_send()


def mode_kernel(
    chunks,
    packed,
    energy_row,
    weight,
    filt,
    modes_out,
    basis_out,
    modes,
    columns,
    lines,
    square_gram,
    store_sem,
):
    count = energy_row.shape[1]
    tall = count * ROWS

    def store(chunk, z):
        rows = pl.ds(pl.multiple_of(chunk * ROWS, ROWS), ROWS)
        return pltpu.make_async_copy(
            modes.at[z, chunk], modes_out.at[:, z, rows, :], store_sem.at[z, chunk]
        )

    square_gram[...] = jnp.zeros_like(square_gram)
    value = packed[...]
    upper = jnp.concatenate(
        [
            value[:, :count],
            jnp.concatenate([value[:, :BLOCK], value[:, count : 2 * count - BLOCK]], axis=1),
            jnp.concatenate(
                [value[:, : 2 * BLOCK], value[:, 2 * count - BLOCK : 2 * count]], axis=1
            ),
        ],
        axis=0,
    )
    shape = (count, count)
    below = lax.broadcasted_iota(jnp.int32, shape, 0) // BLOCK > (
        lax.broadcasted_iota(jnp.int32, shape, 1) // BLOCK
    )
    square_gram[:count, :count] = jnp.where(below, upper.T, upper)
    gram = square_gram[...]

    def eliminate(image, *arrays):
        square = nt(image, image, HIGH)
        for j in range(MODES):
            columns[j] = jnp.broadcast_to(square[:, j : j + 1], (MODES, 128))
        for i, array in enumerate(arrays):
            lines[i] = array
        entry = {
            (i, j): columns[j, i : i + 1, :] for j in range(MODES) for i in range(j, MODES)
        }
        rows = [[lines[n, i : i + 1, :] for i in range(MODES)] for n in range(len(arrays))]
        for k in range(MODES):
            inverse = 1.0 / entry[k, k]
            if k + 1 < MODES:
                side = entry[k + 1, k]
                entry[k + 1, k + 1] = entry[k + 1, k + 1] - (side * side) * inverse
            for i in range(k + 1, MODES):
                factor = entry[i, k] * inverse
                for row in rows:
                    row[i] = row[i] - factor * row[k]
                for j in range(k + 1, i + 1):
                    if (i, j) != (k + 1, k + 1):
                        entry[i, j] = entry[i, j] - factor * entry[j, k]
            scale = lax.rsqrt(entry[k, k])
            for row in rows:
                row[k] = row[k] * scale
        for n, row in enumerate(rows):
            for i in range(MODES):
                lines[n, i : i + 1, :] = row[i]
        return [lines[n] for n in range(len(arrays))]

    def apply(image):
        return jnp.dot(image, gram, precision=HIGH, preferred_element_type=F32)

    image = lax.fori_loop(
        0, ITERS - 1, lambda step, image: eliminate(image, apply(image))[0], gram[:MODES]
    )
    basis, projected = (x[:, :count] for x in eliminate(image, image, apply(image)))
    basis_out[...] = basis
    norms = jnp.sum(basis * projected, axis=1, keepdims=True)
    scaled = basis * energy_row[...] * lax.rsqrt(norms)
    high, low = split(scaled)
    both = jnp.concatenate([high.astype(F32), low.astype(F32)], axis=0).astype(BF16)
    spread = (
        lax.broadcasted_iota(jnp.int32, (count, tall), 0)
        == lax.broadcasted_iota(jnp.int32, (count, tall), 1) // ROWS
    ).astype(F32).astype(BF16)
    both = jnp.dot(both, spread, preferred_element_type=F32)
    both = jnp.broadcast_to(both[:, None, :], (2 * MODES, ROWS, tall))
    keep = lax.broadcasted_iota(jnp.int32, both.shape, 1) == (
        lax.broadcasted_iota(jnp.int32, both.shape, 2) % ROWS
    )
    both = jnp.where(keep, both, 0.0).reshape(2 * MODES * ROWS, tall).astype(BF16)
    top, bottom = both[: MODES * ROWS], both[MODES * ROWS :]
    matrix = jnp.concatenate([top, top, bottom], axis=1)

    def project(step, carry):
        z = step // (chunks // GROUP)
        first = (step % (chunks // GROUP)) * GROUP
        back = lax.rsqrt(jnp.full((1, modes.shape[-1]), weight[z], F32))
        fields = []
        for i in range(GROUP):
            value = filt[z, first + i]
            fields.append(jnp.concatenate([value, value[:tall]], axis=0))
        raw = jnp.dot(
            matrix, jnp.concatenate(fields, axis=1), preferred_element_type=F32
        )
        width = modes.shape[-1]
        for i in range(GROUP):
            part = raw[:, i * width : (i + 1) * width] * back
            modes[z, first + i] = part.reshape(MODES, ROWS, width)
            store(first + i, z).start()
        return carry

    for step in range(4 * chunks // GROUP):
        project(step, 0)
    for z in range(4):
        for chunk in range(chunks):
            store(chunk, z).wait()


def local(snapshots, energies, plane_weight):
    count, planes, rows, width = snapshots.shape
    chunks = rows // ROWS
    cells = planes * 64 * rows * 2 * width
    tall = count * ROWS
    any_space = pl.BlockSpec(memory_space=pl.ANY)
    hbm = pl.BlockSpec(memory_space=pltpu.HBM)
    vmem = pl.BlockSpec(memory_space=pltpu.VMEM)
    smem = pl.BlockSpec(memory_space=pltpu.SMEM)
    dma = pltpu.SemaphoreType.DMA
    filt_shape = (planes, chunks, 2 * tall, width)
    filt, packed = pl.pallas_call(
        functools.partial(gram_kernel, chunks, cells),
        name="gram",
        out_shape=(
            pltpu.VMEM(filt_shape, BF16),
            pltpu.VMEM((BLOCK, 128), F32),
        ),
        in_specs=[hbm, hbm, hbm],
        out_specs=(vmem, vmem),
        scratch_shapes=[
            pltpu.VMEM((chunks, planes, count, ROWS, width), F32),
            pltpu.VMEM((2, chunks, count, ROWS, width), F32),
            pltpu.VMEM((tall, tall), F32),
            pltpu.VMEM((3 * tall, 128), BF16),
            pltpu.VMEM((BLOCK, 128), F32),
            pltpu.VMEM((1, count), F32),
            pltpu.SMEM((planes,), F32),
            pltpu.VMEM((8, BLOCK, 128), F32),
            pltpu.VMEM((16, BLOCK, 128), F32),
            dma((chunks, planes)),
            dma,
            dma,
            dma((2, chunks)),
            dma((2, chunks)),
            dma((8,)),
            dma((8,)),
            dma((16,)),
            dma((16,)),
        ],
        compiler_params=pltpu.CompilerParams(
            collective_id=0, has_side_effects=True, vmem_limit_bytes=VMEM_GRAM
        ),
    )(
        pltpu.with_memory_space_constraint(snapshots, pltpu.HBM),
        pltpu.with_memory_space_constraint(plane_weight, pltpu.HBM),
        pltpu.with_memory_space_constraint(energies[None, :], pltpu.HBM),
    )
    modes, basis = pl.pallas_call(
        functools.partial(mode_kernel, chunks),
        name="modes",
        out_shape=(
            jax.ShapeDtypeStruct((MODES, planes, rows, width), F32),
            jax.ShapeDtypeStruct((MODES, count), F32),
        ),
        in_specs=[vmem, vmem, smem, vmem],
        out_specs=(any_space, vmem),
        scratch_shapes=[
            pltpu.VMEM((planes, chunks, MODES, ROWS, width), F32),
            pltpu.VMEM((MODES, MODES, 128), F32),
            pltpu.VMEM((2, MODES, 128), F32),
            pltpu.VMEM((128, 128), F32),
            dma((planes, chunks)),
        ],
        compiler_params=pltpu.CompilerParams(vmem_limit_bytes=VMEM_MODES),
    )(
        pltpu.with_memory_space_constraint(packed, pltpu.VMEM),
        energies[None, :],
        plane_weight,
        pltpu.with_memory_space_constraint(filt, pltpu.VMEM),
    )
    return modes, basis.T


def solution(mesh):
    torus = Mesh(mesh.devices.reshape(4, 4, 2, 2, mesh.shape["gy"]), NAMES)
    in_specs = (P(None, GZ, "gy", None), P(), P(GZ))
    out_specs = (P(None, GZ, "gy", None), P())
    return jax.shard_map(local, mesh=torus, in_specs=in_specs, out_specs=out_specs, check_vma=False)
```

```python
import functools

import jax
import jax.numpy as jnp
from jax import lax
from jax.experimental import pallas as pl
from jax.experimental.pallas import tpu as pltpu
from jax.sharding import Mesh
from jax.sharding import PartitionSpec as P

MODES = 16
ITERS = 6
NAMES = ("gz_y", "gz_x", "gz_h", "gz_c", "gy")
GZ = NAMES[:4]
MESH = pl.DeviceIdType.MESH
HIGH = lax.Precision.HIGHEST
F32 = jnp.float32
BF16 = jnp.bfloat16
ROWS = 8
BLOCK = 16
GROUP = 4
VMEM_GRAM = 40 * 2**20
VMEM_MODES = 24 * 2**20


def nt(a, b, precision=None):
    return lax.dot_general(
        a, b, (((1,), (1,)), ((), ())), precision=precision, preferred_element_type=F32
    )


def line_device(index):
    return {"gz_h": index // 4, "gz_c": (index // 2) % 2, "gy": index % 2}


def plane_device(index):
    return {"gz_y": index // 4, "gz_x": index % 4}


def slab_device(index):
    return {
        "gz_y": index // 16,
        "gz_x": (index // 4) % 4,
        "gz_h": (index // 2) % 2,
        "gz_c": index % 2,
    }


def split(x):
    high = x.astype(BF16)
    return high, (x - high.astype(F32)).astype(BF16)


def gram_kernel(
    chunks,
    cells,
    snap,
    weight,
    energy_in,
    filt,
    gram_out,
    field,
    halos,
    total,
    choose,
    levels,
    energy_row,
    weights,
    line_buf,
    plane_buf,
    load_sem,
    small_sem,
    energy_sem,
    halo_send,
    halo_recv,
    line_send,
    line_recv,
    plane_send,
    plane_recv,
):
    count = field.shape[2]
    tall = count * ROWS
    y, x, h, c, g = (lax.axis_index(name) for name in NAMES)
    slab = ((y * 4 + x) * 2 + h) * 2 + c
    slabs = 64
    upper = slab_device(lax.rem(slab + 1, slabs))
    lower = slab_device(lax.rem(slab + slabs - 1, slabs))
    line = (h * 2 + c) * 2 + g
    plane = y * 4 + x

    barrier = pltpu.get_barrier_semaphore()
    for device in (upper, lower):
        pl.semaphore_signal(barrier, inc=1, device_id=device, device_id_type=MESH)
    for step in range(1, 8):
        device = line_device(lax.rem(line + step, 8))
        pl.semaphore_signal(barrier, inc=1, device_id=device, device_id_type=MESH)
    for step in range(1, 16):
        device = plane_device(lax.rem(plane + step, 16))
        pl.semaphore_signal(barrier, inc=1, device_id=device, device_id_type=MESH)

    def load(chunk, z):
        rows = pl.ds(pl.multiple_of(chunk * ROWS, ROWS), ROWS)
        return pltpu.make_async_copy(
            snap.at[:, z, rows, :], field.at[chunk, z], load_sem.at[chunk, z]
        )

    def halo(chunk, side):
        return pltpu.make_async_remote_copy(
            src_ref=field.at[chunk, 3 if side == 0 else 0],
            dst_ref=halos.at[side, chunk],
            send_sem=halo_send.at[side, chunk],
            recv_sem=halo_recv.at[side, chunk],
            device_id=upper if side == 0 else lower,
            device_id_type=MESH,
        )

    def arrival(chunk, side):
        return pltpu.make_async_remote_copy(
            src_ref=halos.at[side, chunk],
            dst_ref=halos.at[side, chunk],
            send_sem=halo_send.at[side, chunk],
            recv_sem=halo_recv.at[side, chunk],
            device_id=upper,
            device_id_type=MESH,
        )

    for chunk in range(chunks):
        for z in (3, 0):
            load(chunk, z).start()
    for chunk in range(chunks):
        for z in (1, 2):
            load(chunk, z).start()
    read = pltpu.make_async_copy(weight, weights, small_sem)
    read.start()
    fetch = pltpu.make_async_copy(energy_in, energy_row, energy_sem)
    fetch.start()
    pl.semaphore_wait(barrier, 24)
    for chunk in range(chunks):
        for side in range(2):
            load(chunk, 3 if side == 0 else 0).wait()
            halo(chunk, side).start()
    read.wait()
    fetch.wait()
    total[...] = jnp.zeros_like(total)
    place = lax.broadcasted_iota(jnp.int32, (3 * tall, 128), 0) // ROWS
    lane = lax.broadcasted_iota(jnp.int32, (3 * tall, 128), 1)
    second, third = place - count, place - 2 * count
    second = jnp.where(second >= BLOCK, second + 2 * BLOCK, -1)
    third = jnp.where(third >= 2 * BLOCK, third + 3 * BLOCK, -1)
    target = jnp.where(place < count, place, jnp.where(place < 2 * count, second, third))
    choose[...] = (target == lane).astype(F32).astype(BF16)

    energy = energy_row[...]
    across = jnp.concatenate(
        [energy, energy[:, BLOCK:], energy[:, 2 * BLOCK :], jnp.zeros((1, 2 * BLOCK), F32)],
        axis=1,
    )
    down = jnp.broadcast_to(energy, (128, count)).T
    lane = lax.broadcasted_iota(jnp.int32, (BLOCK, 128), 1)
    down = jnp.where(
        lane < count,
        down[:BLOCK],
        jnp.where(lane < 2 * count - BLOCK, down[BLOCK : 2 * BLOCK], down[2 * BLOCK :]),
    )
    levels[...] = down * across * (1.0 / cells)

    def smooth(a, b, c, z):
        root = jnp.sqrt(jnp.full((1, 256), weights[z], F32))
        return (0.25 * root) * (a + c) + (0.5 * root) * b

    def accumulate(chunk, planes, values):
        highs, lows = [], []
        for z, value in zip(planes, values):
            high, low = split(value)
            filt[z, chunk, :tall, :] = high
            filt[z, chunk, tall:, :] = low
            highs.append(high)
            lows.append(low)
        high = jnp.concatenate(highs, axis=1)
        low = jnp.concatenate(lows, axis=1)
        total[...] += nt(
            jnp.concatenate([high, high, low], axis=1),
            jnp.concatenate([high, low, high], axis=1),
        )

    def flat(ref):
        return ref[...].reshape(tall, ref.shape[-1])

    def inner(chunk, carry):
        for z in (1, 2):
            load(chunk, z).wait()
        s = [flat(field.at[chunk, z]) for z in range(4)]
        accumulate(
            chunk, (1, 2), [smooth(s[0], s[1], s[2], 1), smooth(s[1], s[2], s[3], 2)]
        )
        return carry

    lax.fori_loop(0, chunks, inner, 0)

    for side in (1 - c, c * 1):
        z = side * 3

        def outer(chunk, carry, side=side, z=z):
            arrival(chunk, side).wait_recv()
            value = smooth(
                flat(halos.at[side, chunk]),
                flat(field.at[chunk, z]),
                flat(field.at[chunk, 1 + side]),
                z,
            )
            accumulate(chunk, (z,), [value])
            return carry

        for chunk in range(chunks):
            outer(chunk, 0)

    keep = lax.broadcasted_iota(jnp.int32, (tall, tall), 0) % ROWS == (
        lax.broadcasted_iota(jnp.int32, (tall, tall), 1) % ROWS
    )
    picked = jnp.sum(
        jnp.where(keep, total[...], 0.0).reshape(count, ROWS, tall), axis=1
    )
    rest = jnp.concatenate(
        [picked[:BLOCK], picked[BLOCK : 2 * BLOCK], picked[2 * BLOCK :]], axis=1
    )
    pieces = []
    for part in range(3):
        piece = rest.astype(BF16).astype(F32)
        rest = rest - piece
        pieces.append(piece)
    pieces = jnp.concatenate(pieces, axis=0).astype(BF16)
    pieces = jnp.dot(pieces, choose[...], preferred_element_type=F32)
    packed = pieces[:BLOCK] + pieces[BLOCK : 2 * BLOCK] + pieces[2 * BLOCK :]

    def reduce(value, buf, me, size, device_of, send, recv, order, shift):
        buf[me] = value
        copies = []
        for offset in order:
            other = shift(offset)
            copies.append(
                pltpu.make_async_remote_copy(
                    src_ref=buf.at[me],
                    dst_ref=buf.at[me],
                    send_sem=send.at[other],
                    recv_sem=recv.at[me],
                    device_id=device_of(other),
                    device_id_type=MESH,
                )
            )
        for copy in copies:
            copy.start()
        for offset in order:
            other = shift(offset)
            pltpu.make_async_remote_copy(
                src_ref=buf.at[other],
                dst_ref=buf.at[other],
                send_sem=send.at[other],
                recv_sem=recv.at[other],
                device_id=device_of(other),
                device_id_type=MESH,
            ).wait_recv()
        parts = [buf[i] for i in range(size)]
        while len(parts) > 1:
            parts = [parts[i] + parts[i + 1] for i in range(0, len(parts), 2)]
        return parts[0], copies

    packed, line_copies = reduce(
        packed, line_buf, line, 8, line_device, line_send, line_recv,
        [(1, 1, 0), (1, 0, 0), (1, 1, 1), (0, 1, 1), (1, 0, 1), (0, 0, 1), (0, 1, 0)],
        lambda o: (lax.rem(h + o[0], 2) * 2 + lax.rem(c + o[1], 2)) * 2 + lax.rem(g + o[2], 2),
    )
    packed, plane_copies = reduce(
        packed, plane_buf, plane, 16, plane_device, plane_send, plane_recv,
        sorted(
            [(i, j) for i in range(4) for j in range(4) if i or j],
            key=lambda o: -(min(o[0], 4 - o[0]) + min(o[1], 4 - o[1])),
        ),
        lambda o: lax.rem(y + o[0], 4) * 4 + lax.rem(x + o[1], 4),
    )
    gram_out[...] = packed * levels[...]
    for copy in line_copies + plane_copies:
        copy.wait_send()
    for chunk in range(chunks):
        for side in range(2):
            halo(chunk, side).wait_send()


def mode_kernel(
    chunks,
    packed,
    energy_row,
    weight,
    filt,
    modes_out,
    basis_out,
    modes,
    columns,
    lines,
    square_gram,
    store_sem,
):
    count = energy_row.shape[1]
    tall = count * ROWS

    def store(chunk, z):
        rows = pl.ds(pl.multiple_of(chunk * ROWS, ROWS), ROWS)
        return pltpu.make_async_copy(
            modes.at[z, chunk], modes_out.at[:, z, rows, :], store_sem.at[z, chunk]
        )

    square_gram[...] = jnp.zeros_like(square_gram)
    value = packed[...]
    upper = jnp.concatenate(
        [
            value[:, :count],
            jnp.concatenate([value[:, :BLOCK], value[:, count : 2 * count - BLOCK]], axis=1),
            jnp.concatenate(
                [value[:, : 2 * BLOCK], value[:, 2 * count - BLOCK : 2 * count]], axis=1
            ),
        ],
        axis=0,
    )
    shape = (count, count)
    below = lax.broadcasted_iota(jnp.int32, shape, 0) // BLOCK > (
        lax.broadcasted_iota(jnp.int32, shape, 1) // BLOCK
    )
    square_gram[:count, :count] = jnp.where(below, upper.T, upper)
    gram = square_gram[...]

    def eliminate(image, *arrays):
        square = nt(image, image, HIGH)
        for j in range(MODES):
            columns[j] = jnp.broadcast_to(square[:, j : j + 1], (MODES, 128))
        for i, array in enumerate(arrays):
            lines[i] = array
        entry = {
            (i, j): columns[j, i : i + 1, :] for j in range(MODES) for i in range(j, MODES)
        }
        rows = [[lines[n, i : i + 1, :] for i in range(MODES)] for n in range(len(arrays))]
        for k in range(MODES):
            inverse = 1.0 / entry[k, k]
            if k + 1 < MODES:
                side = entry[k + 1, k]
                entry[k + 1, k + 1] = entry[k + 1, k + 1] - (side * side) * inverse
            for i in range(k + 1, MODES):
                factor = entry[i, k] * inverse
                for row in rows:
                    row[i] = row[i] - factor * row[k]
                for j in range(k + 1, i + 1):
                    if (i, j) != (k + 1, k + 1):
                        entry[i, j] = entry[i, j] - factor * entry[j, k]
            scale = lax.rsqrt(entry[k, k])
            for row in rows:
                row[k] = row[k] * scale
        for n, row in enumerate(rows):
            for i in range(MODES):
                lines[n, i : i + 1, :] = row[i]
        return [lines[n] for n in range(len(arrays))]

    def apply(image):
        return jnp.dot(image, gram, precision=HIGH, preferred_element_type=F32)

    image = lax.fori_loop(
        0, ITERS - 1, lambda step, image: eliminate(image, apply(image))[0], gram[:MODES]
    )
    basis, projected = (x[:, :count] for x in eliminate(image, image, apply(image)))
    basis_out[...] = basis
    norms = jnp.sum(basis * projected, axis=1, keepdims=True)
    scaled = basis * energy_row[...] * lax.rsqrt(norms)
    high, low = split(scaled)
    both = jnp.concatenate([high.astype(F32), low.astype(F32)], axis=0).astype(BF16)
    spread = (
        lax.broadcasted_iota(jnp.int32, (count, tall), 0)
        == lax.broadcasted_iota(jnp.int32, (count, tall), 1) // ROWS
    ).astype(F32).astype(BF16)
    both = jnp.dot(both, spread, preferred_element_type=F32)
    both = jnp.broadcast_to(both[:, None, :], (2 * MODES, ROWS, tall))
    keep = lax.broadcasted_iota(jnp.int32, both.shape, 1) == (
        lax.broadcasted_iota(jnp.int32, both.shape, 2) % ROWS
    )
    both = jnp.where(keep, both, 0.0).reshape(2 * MODES * ROWS, tall).astype(BF16)
    top, bottom = both[: MODES * ROWS], both[MODES * ROWS :]
    matrix = jnp.concatenate([top, top, bottom], axis=1)

    def project(step, carry):
        z = step // (chunks // GROUP)
        first = (step % (chunks // GROUP)) * GROUP
        back = lax.rsqrt(jnp.full((1, modes.shape[-1]), weight[z], F32))
        fields = []
        for i in range(GROUP):
            value = filt[z, first + i]
            fields.append(jnp.concatenate([value, value[:tall]], axis=0))
        raw = jnp.dot(
            matrix, jnp.concatenate(fields, axis=1), preferred_element_type=F32
        )
        width = modes.shape[-1]
        for i in range(GROUP):
            part = raw[:, i * width : (i + 1) * width] * back
            modes[z, first + i] = part.reshape(MODES, ROWS, width)
            store(first + i, z).start()
        return carry

    for step in range(4 * chunks // GROUP):
        project(step, 0)
    for z in range(4):
        for chunk in range(chunks):
            store(chunk, z).wait()


def local(snapshots, energies, plane_weight):
    count, planes, rows, width = snapshots.shape
    chunks = rows // ROWS
    cells = planes * 64 * rows * 2 * width
    tall = count * ROWS
    any_space = pl.BlockSpec(memory_space=pl.ANY)
    hbm = pl.BlockSpec(memory_space=pltpu.HBM)
    vmem = pl.BlockSpec(memory_space=pltpu.VMEM)
    smem = pl.BlockSpec(memory_space=pltpu.SMEM)
    dma = pltpu.SemaphoreType.DMA
    filt_shape = (planes, chunks, 2 * tall, width)
    filt, packed = pl.pallas_call(
        functools.partial(gram_kernel, chunks, cells),
        name="gram",
        out_shape=(
            pltpu.VMEM(filt_shape, BF16),
            pltpu.VMEM((BLOCK, 128), F32),
        ),
        in_specs=[hbm, hbm, hbm],
        out_specs=(vmem, vmem),
        scratch_shapes=[
            pltpu.VMEM((chunks, planes, count, ROWS, width), F32),
            pltpu.VMEM((2, chunks, count, ROWS, width), F32),
            pltpu.VMEM((tall, tall), F32),
            pltpu.VMEM((3 * tall, 128), BF16),
            pltpu.VMEM((BLOCK, 128), F32),
            pltpu.VMEM((1, count), F32),
            pltpu.SMEM((planes,), F32),
            pltpu.VMEM((8, BLOCK, 128), F32),
            pltpu.VMEM((16, BLOCK, 128), F32),
            dma((chunks, planes)),
            dma,
            dma,
            dma((2, chunks)),
            dma((2, chunks)),
            dma((8,)),
            dma((8,)),
            dma((16,)),
            dma((16,)),
        ],
        compiler_params=pltpu.CompilerParams(
            collective_id=0, has_side_effects=True, vmem_limit_bytes=VMEM_GRAM
        ),
    )(
        pltpu.with_memory_space_constraint(snapshots, pltpu.HBM),
        pltpu.with_memory_space_constraint(plane_weight, pltpu.HBM),
        pltpu.with_memory_space_constraint(energies[None, :], pltpu.HBM),
    )
    modes, basis = pl.pallas_call(
        functools.partial(mode_kernel, chunks),
        name="modes",
        out_shape=(
            jax.ShapeDtypeStruct((MODES, planes, rows, width), F32),
            jax.ShapeDtypeStruct((MODES, count), F32),
        ),
        in_specs=[vmem, vmem, smem, vmem],
        out_specs=(any_space, vmem),
        scratch_shapes=[
            pltpu.VMEM((planes, chunks, MODES, ROWS, width), F32),
            pltpu.VMEM((MODES, MODES, 128), F32),
            pltpu.VMEM((2, MODES, 128), F32),
            pltpu.VMEM((128, 128), F32),
            dma((planes, chunks)),
        ],
        compiler_params=pltpu.CompilerParams(vmem_limit_bytes=VMEM_MODES),
    )(
        pltpu.with_memory_space_constraint(packed, pltpu.VMEM),
        energies[None, :],
        plane_weight,
        pltpu.with_memory_space_constraint(filt, pltpu.VMEM),
    )
    return modes, basis.T


def solution(mesh):
    torus = Mesh(mesh.devices.reshape(4, 4, 2, 2, mesh.shape["gy"]), NAMES)
    in_specs = (P(None, GZ, "gy", None), P(), P(GZ))
    out_specs = (P(None, GZ, "gy", None), P())
    return jax.shard_map(local, mesh=torus, in_specs=in_specs, out_specs=out_specs, check_vma=False)
```

```python
import functools

import jax
import jax.numpy as jnp
from jax import lax
from jax.experimental import pallas as pl
from jax.experimental.pallas import tpu as pltpu
from jax.sharding import Mesh
from jax.sharding import PartitionSpec as P

MODES = 16
ITERS = 6
NAMES = ("gz_y", "gz_x", "gz_h", "gz_c", "gy")
GZ = NAMES[:4]
MESH = pl.DeviceIdType.MESH
HIGH = lax.Precision.HIGHEST
F32 = jnp.float32
BF16 = jnp.bfloat16
ROWS = 8
BLOCK = 16
GROUP = 4
VMEM_GRAM = 40 * 2**20
VMEM_MODES = 24 * 2**20


def nt(a, b, precision=None):
    return lax.dot_general(
        a, b, (((1,), (1,)), ((), ())), precision=precision, preferred_element_type=F32
    )


def line_device(index):
    return {"gz_h": index // 4, "gz_c": (index // 2) % 2, "gy": index % 2}


def plane_device(index):
    return {"gz_y": index // 4, "gz_x": index % 4}


def slab_device(index):
    return {
        "gz_y": index // 16,
        "gz_x": (index // 4) % 4,
        "gz_h": (index // 2) % 2,
        "gz_c": index % 2,
    }


def split(x):
    high = x.astype(BF16)
    return high, (x - high.astype(F32)).astype(BF16)


def gram_kernel(
    chunks,
    cells,
    snap,
    weight,
    energy_in,
    filt,
    gram_out,
    field,
    halos,
    total,
    choose,
    levels,
    energy_row,
    weights,
    line_buf,
    plane_buf,
    load_sem,
    small_sem,
    energy_sem,
    halo_send,
    halo_recv,
    line_send,
    line_recv,
    plane_send,
    plane_recv,
):
    count = field.shape[2]
    tall = count * ROWS
    y, x, h, c, g = (lax.axis_index(name) for name in NAMES)
    slab = ((y * 4 + x) * 2 + h) * 2 + c
    slabs = 64
    upper = slab_device(lax.rem(slab + 1, slabs))
    lower = slab_device(lax.rem(slab + slabs - 1, slabs))
    line = (h * 2 + c) * 2 + g
    plane = y * 4 + x

    barrier = pltpu.get_barrier_semaphore()
    for device in (upper, lower):
        pl.semaphore_signal(barrier, inc=1, device_id=device, device_id_type=MESH)
    for step in range(1, 8):
        device = line_device(lax.rem(line + step, 8))
        pl.semaphore_signal(barrier, inc=1, device_id=device, device_id_type=MESH)
    for step in range(1, 16):
        device = plane_device(lax.rem(plane + step, 16))
        pl.semaphore_signal(barrier, inc=1, device_id=device, device_id_type=MESH)

    def load(chunk, z):
        rows = pl.ds(pl.multiple_of(chunk * ROWS, ROWS), ROWS)
        return pltpu.make_async_copy(
            snap.at[:, z, rows, :], field.at[chunk, z], load_sem.at[chunk, z]
        )

    def halo(chunk, side):
        return pltpu.make_async_remote_copy(
            src_ref=field.at[chunk, 3 if side == 0 else 0],
            dst_ref=halos.at[side, chunk],
            send_sem=halo_send.at[side, chunk],
            recv_sem=halo_recv.at[side, chunk],
            device_id=upper if side == 0 else lower,
            device_id_type=MESH,
        )

    def arrival(chunk, side):
        return pltpu.make_async_remote_copy(
            src_ref=halos.at[side, chunk],
            dst_ref=halos.at[side, chunk],
            send_sem=halo_send.at[side, chunk],
            recv_sem=halo_recv.at[side, chunk],
            device_id=upper,
            device_id_type=MESH,
        )

    for chunk in range(chunks):
        for z in (3, 0):
            load(chunk, z).start()
    for chunk in range(chunks):
        for z in (1, 2):
            load(chunk, z).start()
    read = pltpu.make_async_copy(weight, weights, small_sem)
    read.start()
    fetch = pltpu.make_async_copy(energy_in, energy_row, energy_sem)
    fetch.start()
    pl.semaphore_wait(barrier, 24)
    for chunk in range(chunks):
        for side in range(2):
            load(chunk, 3 if side == 0 else 0).wait()
            halo(chunk, side).start()
    read.wait()
    fetch.wait()
    total[...] = jnp.zeros_like(total)
    place = lax.broadcasted_iota(jnp.int32, (3 * tall, 128), 0) // ROWS
    lane = lax.broadcasted_iota(jnp.int32, (3 * tall, 128), 1)
    second, third = place - count, place - 2 * count
    second = jnp.where(second >= BLOCK, second + 2 * BLOCK, -1)
    third = jnp.where(third >= 2 * BLOCK, third + 3 * BLOCK, -1)
    target = jnp.where(place < count, place, jnp.where(place < 2 * count, second, third))
    choose[...] = (target == lane).astype(F32).astype(BF16)

    energy = energy_row[...]
    across = jnp.concatenate(
        [energy, energy[:, BLOCK:], energy[:, 2 * BLOCK :], jnp.zeros((1, 2 * BLOCK), F32)],
        axis=1,
    )
    down = jnp.broadcast_to(energy, (128, count)).T
    lane = lax.broadcasted_iota(jnp.int32, (BLOCK, 128), 1)
    down = jnp.where(
        lane < count,
        down[:BLOCK],
        jnp.where(lane < 2 * count - BLOCK, down[BLOCK : 2 * BLOCK], down[2 * BLOCK :]),
    )
    levels[...] = down * across * (1.0 / cells)

    def smooth(a, b, c, z):
        root = jnp.sqrt(jnp.full((1, 256), weights[z], F32))
        return (0.25 * root) * (a + c) + (0.5 * root) * b

    def accumulate(chunk, planes, values):
        highs, lows = [], []
        for z, value in zip(planes, values):
            high, low = split(value)
            filt[z, chunk, :tall, :] = high
            filt[z, chunk, tall:, :] = low
            highs.append(high)
            lows.append(low)
        high = jnp.concatenate(highs, axis=1)
        low = jnp.concatenate(lows, axis=1)
        total[...] += nt(
            jnp.concatenate([high, high, low, low], axis=1),
            jnp.concatenate([high, low, high, low], axis=1),
        )

    def flat(ref):
        return ref[...].reshape(tall, ref.shape[-1])

    def inner(chunk, carry):
        for z in (1, 2):
            load(chunk, z).wait()
        s = [flat(field.at[chunk, z]) for z in range(4)]
        accumulate(
            chunk, (1, 2), [smooth(s[0], s[1], s[2], 1), smooth(s[1], s[2], s[3], 2)]
        )
        return carry

    lax.fori_loop(0, chunks, inner, 0)

    for side in (1 - c, c * 1):
        z = side * 3

        def outer(chunk, carry, side=side, z=z):
            arrival(chunk, side).wait_recv()
            value = smooth(
                flat(halos.at[side, chunk]),
                flat(field.at[chunk, z]),
                flat(field.at[chunk, 1 + side]),
                z,
            )
            accumulate(chunk, (z,), [value])
            return carry

        for chunk in range(chunks):
            outer(chunk, 0)

    keep = lax.broadcasted_iota(jnp.int32, (tall, tall), 0) % ROWS == (
        lax.broadcasted_iota(jnp.int32, (tall, tall), 1) % ROWS
    )
    picked = jnp.sum(
        jnp.where(keep, total[...], 0.0).reshape(count, ROWS, tall), axis=1
    )
    rest = jnp.concatenate(
        [picked[:BLOCK], picked[BLOCK : 2 * BLOCK], picked[2 * BLOCK :]], axis=1
    )
    pieces = []
    for part in range(3):
        piece = rest.astype(BF16).astype(F32)
        rest = rest - piece
        pieces.append(piece)
    pieces = jnp.concatenate(pieces, axis=0).astype(BF16)
    pieces = jnp.dot(pieces, choose[...], preferred_element_type=F32)
    packed = pieces[:BLOCK] + pieces[BLOCK : 2 * BLOCK] + pieces[2 * BLOCK :]

    def reduce(value, buf, me, size, device_of, send, recv, order, shift):
        buf[me] = value
        copies = []
        for offset in order:
            other = shift(offset)
            copies.append(
                pltpu.make_async_remote_copy(
                    src_ref=buf.at[me],
                    dst_ref=buf.at[me],
                    send_sem=send.at[other],
                    recv_sem=recv.at[me],
                    device_id=device_of(other),
                    device_id_type=MESH,
                )
            )
        for copy in copies:
            copy.start()
        for offset in order:
            other = shift(offset)
            pltpu.make_async_remote_copy(
                src_ref=buf.at[other],
                dst_ref=buf.at[other],
                send_sem=send.at[other],
                recv_sem=recv.at[other],
                device_id=device_of(other),
                device_id_type=MESH,
            ).wait_recv()
        parts = [buf[i] for i in range(size)]
        while len(parts) > 1:
            parts = [parts[i] + parts[i + 1] for i in range(0, len(parts), 2)]
        return parts[0], copies

    packed, line_copies = reduce(
        packed, line_buf, line, 8, line_device, line_send, line_recv,
        [(1, 1, 0), (1, 0, 0), (1, 1, 1), (0, 1, 1), (1, 0, 1), (0, 0, 1), (0, 1, 0)],
        lambda o: (lax.rem(h + o[0], 2) * 2 + lax.rem(c + o[1], 2)) * 2 + lax.rem(g + o[2], 2),
    )
    packed, plane_copies = reduce(
        packed, plane_buf, plane, 16, plane_device, plane_send, plane_recv,
        sorted(
            [(i, j) for i in range(4) for j in range(4) if i or j],
            key=lambda o: -(min(o[0], 4 - o[0]) + min(o[1], 4 - o[1])),
        ),
        lambda o: lax.rem(y + o[0], 4) * 4 + lax.rem(x + o[1], 4),
    )
    gram_out[...] = packed * levels[...]
    for copy in line_copies + plane_copies:
        copy.wait_send()
    for chunk in range(chunks):
        for side in range(2):
            halo(chunk, side).wait_send()


def mode_kernel(
    chunks,
    packed,
    energy_row,
    weight,
    filt,
    modes_out,
    basis_out,
    modes,
    columns,
    lines,
    square_gram,
    store_sem,
):
    count = energy_row.shape[1]
    tall = count * ROWS

    def store(chunk, z):
        rows = pl.ds(pl.multiple_of(chunk * ROWS, ROWS), ROWS)
        return pltpu.make_async_copy(
            modes.at[z, chunk], modes_out.at[:, z, rows, :], store_sem.at[z, chunk]
        )

    square_gram[...] = jnp.zeros_like(square_gram)
    value = packed[...]
    upper = jnp.concatenate(
        [
            value[:, :count],
            jnp.concatenate([value[:, :BLOCK], value[:, count : 2 * count - BLOCK]], axis=1),
            jnp.concatenate(
                [value[:, : 2 * BLOCK], value[:, 2 * count - BLOCK : 2 * count]], axis=1
            ),
        ],
        axis=0,
    )
    shape = (count, count)
    below = lax.broadcasted_iota(jnp.int32, shape, 0) // BLOCK > (
        lax.broadcasted_iota(jnp.int32, shape, 1) // BLOCK
    )
    square_gram[:count, :count] = jnp.where(below, upper.T, upper)
    gram = square_gram[...]

    def eliminate(image, *arrays):
        square = nt(image, image, HIGH)
        for j in range(MODES):
            columns[j] = jnp.broadcast_to(square[:, j : j + 1], (MODES, 128))
        for i, array in enumerate(arrays):
            lines[i] = array
        entry = {
            (i, j): columns[j, i : i + 1, :] for j in range(MODES) for i in range(j, MODES)
        }
        rows = [[lines[n, i : i + 1, :] for i in range(MODES)] for n in range(len(arrays))]
        for k in range(MODES):
            inverse = 1.0 / entry[k, k]
            if k + 1 < MODES:
                side = entry[k + 1, k]
                entry[k + 1, k + 1] = entry[k + 1, k + 1] - (side * side) * inverse
            for i in range(k + 1, MODES):
                factor = entry[i, k] * inverse
                for row in rows:
                    row[i] = row[i] - factor * row[k]
                for j in range(k + 1, i + 1):
                    if (i, j) != (k + 1, k + 1):
                        entry[i, j] = entry[i, j] - factor * entry[j, k]
            scale = lax.rsqrt(entry[k, k])
            for row in rows:
                row[k] = row[k] * scale
        for n, row in enumerate(rows):
            for i in range(MODES):
                lines[n, i : i + 1, :] = row[i]
        return [lines[n] for n in range(len(arrays))]

    def apply(image):
        return jnp.dot(image, gram, precision=HIGH, preferred_element_type=F32)

    image = lax.fori_loop(
        0, ITERS - 1, lambda step, image: eliminate(image, apply(image))[0], gram[:MODES]
    )
    basis, projected = (x[:, :count] for x in eliminate(image, image, apply(image)))
    basis_out[...] = basis
    norms = jnp.sum(basis * projected, axis=1, keepdims=True)
    scaled = basis * energy_row[...] * lax.rsqrt(norms)
    high, low = split(scaled)
    both = jnp.concatenate([high.astype(F32), low.astype(F32)], axis=0).astype(BF16)
    spread = (
        lax.broadcasted_iota(jnp.int32, (count, tall), 0)
        == lax.broadcasted_iota(jnp.int32, (count, tall), 1) // ROWS
    ).astype(F32).astype(BF16)
    both = jnp.dot(both, spread, preferred_element_type=F32)
    both = jnp.broadcast_to(both[:, None, :], (2 * MODES, ROWS, tall))
    keep = lax.broadcasted_iota(jnp.int32, both.shape, 1) == (
        lax.broadcasted_iota(jnp.int32, both.shape, 2) % ROWS
    )
    both = jnp.where(keep, both, 0.0).reshape(2 * MODES * ROWS, tall).astype(BF16)
    top, bottom = both[: MODES * ROWS], both[MODES * ROWS :]
    matrix = jnp.concatenate([top, top, bottom], axis=1)

    def project(step, carry):
        z = step // (chunks // GROUP)
        first = (step % (chunks // GROUP)) * GROUP
        back = lax.rsqrt(jnp.full((1, modes.shape[-1]), weight[z], F32))
        fields = []
        for i in range(GROUP):
            value = filt[z, first + i]
            fields.append(jnp.concatenate([value, value[:tall]], axis=0))
        raw = jnp.dot(
            matrix, jnp.concatenate(fields, axis=1), preferred_element_type=F32
        )
        width = modes.shape[-1]
        for i in range(GROUP):
            part = raw[:, i * width : (i + 1) * width] * back
            modes[z, first + i] = part.reshape(MODES, ROWS, width)
            store(first + i, z).start()
        return carry

    for step in range(4 * chunks // GROUP):
        project(step, 0)
    for z in range(4):
        for chunk in range(chunks):
            store(chunk, z).wait()


def local(snapshots, energies, plane_weight):
    count, planes, rows, width = snapshots.shape
    chunks = rows // ROWS
    cells = planes * 64 * rows * 2 * width
    tall = count * ROWS
    any_space = pl.BlockSpec(memory_space=pl.ANY)
    hbm = pl.BlockSpec(memory_space=pltpu.HBM)
    vmem = pl.BlockSpec(memory_space=pltpu.VMEM)
    smem = pl.BlockSpec(memory_space=pltpu.SMEM)
    dma = pltpu.SemaphoreType.DMA
    filt_shape = (planes, chunks, 2 * tall, width)
    filt, packed = pl.pallas_call(
        functools.partial(gram_kernel, chunks, cells),
        name="gram",
        out_shape=(
            pltpu.VMEM(filt_shape, BF16),
            pltpu.VMEM((BLOCK, 128), F32),
        ),
        in_specs=[hbm, hbm, hbm],
        out_specs=(vmem, vmem),
        scratch_shapes=[
            pltpu.VMEM((chunks, planes, count, ROWS, width), F32),
            pltpu.VMEM((2, chunks, count, ROWS, width), F32),
            pltpu.VMEM((tall, tall), F32),
            pltpu.VMEM((3 * tall, 128), BF16),
            pltpu.VMEM((BLOCK, 128), F32),
            pltpu.VMEM((1, count), F32),
            pltpu.SMEM((planes,), F32),
            pltpu.VMEM((8, BLOCK, 128), F32),
            pltpu.VMEM((16, BLOCK, 128), F32),
            dma((chunks, planes)),
            dma,
            dma,
            dma((2, chunks)),
            dma((2, chunks)),
            dma((8,)),
            dma((8,)),
            dma((16,)),
            dma((16,)),
        ],
        compiler_params=pltpu.CompilerParams(
            collective_id=0, has_side_effects=True, vmem_limit_bytes=VMEM_GRAM
        ),
    )(
        pltpu.with_memory_space_constraint(snapshots, pltpu.HBM),
        pltpu.with_memory_space_constraint(plane_weight, pltpu.HBM),
        pltpu.with_memory_space_constraint(energies[None, :], pltpu.HBM),
    )
    modes, basis = pl.pallas_call(
        functools.partial(mode_kernel, chunks),
        name="modes",
        out_shape=(
            jax.ShapeDtypeStruct((MODES, planes, rows, width), F32),
            jax.ShapeDtypeStruct((MODES, count), F32),
        ),
        in_specs=[vmem, vmem, smem, vmem],
        out_specs=(any_space, vmem),
        scratch_shapes=[
            pltpu.VMEM((planes, chunks, MODES, ROWS, width), F32),
            pltpu.VMEM((MODES, MODES, 128), F32),
            pltpu.VMEM((2, MODES, 128), F32),
            pltpu.VMEM((128, 128), F32),
            dma((planes, chunks)),
        ],
        compiler_params=pltpu.CompilerParams(vmem_limit_bytes=VMEM_MODES),
    )(
        pltpu.with_memory_space_constraint(packed, pltpu.VMEM),
        energies[None, :],
        plane_weight,
        pltpu.with_memory_space_constraint(filt, pltpu.VMEM),
    )
    return modes, basis.T


def solution(mesh):
    torus = Mesh(mesh.devices.reshape(4, 4, 2, 2, mesh.shape["gy"]), NAMES)
    in_specs = (P(None, GZ, "gy", None), P(), P(GZ))
    out_specs = (P(None, GZ, "gy", None), P())
    return jax.shard_map(local, mesh=torus, in_specs=in_specs, out_specs=out_specs, check_vma=False)
```
